32 devices in a mesh: rep: 1 (over z), dp: 32 (over x, y, core).
Axes of the slice: x: 4, y: 4, z: 1, core: 2. Of those that a mesh axis runs over, the one named last changes fastest.
The devices are a block of a 4x4x8 slice.
Arguments:
- x: bfloat16 [32, 2048, 1024], P(('rep', 'dp'))
- dy: bfloat16 [32, 2048, 1024], P(('rep', 'dp'))
- w_gate: bfloat16 [2, 1024, 2816], P(None, 'dp')
- w_up: bfloat16 [2, 1024, 2816], P(None, 'dp')
- w_down: bfloat16 [2, 2816, 1024], P(None, 'dp')
- m_w_gate: float32 [2, 1024, 2816], P(None, 'dp')
- m_w_up: float32 [2, 1024, 2816], P(None, 'dp')
- m_w_down: float32 [2, 2816, 1024], P(None, 'dp')
- v_w_gate: float32 [2, 1024, 2816], P(None, 'dp')
- v_w_up: float32 [2, 1024, 2816], P(None, 'dp')
- v_w_down: float32 [2, 2816, 1024], P(None, 'dp')
Outputs:
- output 1: bfloat16 [2, 1024, 2816], P('rep', 'dp')
- output 2: bfloat16 [2, 1024, 2816], P('rep', 'dp')
- output 3: bfloat16 [2, 2816, 1024], P('rep', 'dp')
- output 4: float32 [2, 1024, 2816], P('rep', 'dp')
- output 5: float32 [2, 1024, 2816], P('rep', 'dp')
- output 6: float32 [2, 2816, 1024], P('rep', 'dp')
- output 7: float32 [2, 1024, 2816], P('rep', 'dp')
- output 8: float32 [2, 1024, 2816], P('rep', 'dp')
- output 9: float32 [2, 2816, 1024], P('rep', 'dp')
All inputs are finite; a program needn't handle non-finite values.
Results may differ from the reference program's by a relative error of at most 0.022.
Values are sent between devices in bfloat16 or wider.
A program may use at most 768 MiB of HBM per device.

```python
import jax
import jax.numpy as jnp
from jax import lax

SEQUENCES = 32
TOKENS = 2048
D = 1024
FF = 2816
LAYERS = 2
NAMES = ("w_gate", "w_up", "w_down")
SHAPES = {"w_gate": (LAYERS, D, FF), "w_up": (LAYERS, D, FF), "w_down": (LAYERS, FF, D)}


def bump(key, n, height):
    away = (jnp.arange(n, dtype=jnp.int32) - jax.random.randint(key, (), 0, n, jnp.int32)) % n
    return jnp.where(away < n // 8, height, 1.0)


def together(key, own, strength):
    shared = jax.random.normal(key, own.shape[1:], jnp.float32)
    return (own + strength * shared) * lax.rsqrt(1 + strength * strength)


def setup_inputs(seed: int = 0, part: int = 0) -> dict:
    kx, kdy, ka, kb, kz, kf, kh, kl, *keys = jax.random.split(jax.random.key(seed), 8 + 3 * len(NAMES))
    kx, kdy, ka, kb = (jax.random.fold_in(k, part) for k in (kx, kdy, ka, kb))
    kw, km, kv = (keys[i::3] for i in range(3))
    shape = (SEQUENCES, TOKENS, D)
    much_x, much_dy = jax.random.uniform(kz, (2,), jnp.float32, 0.0, 1.0)
    loud = 2.0 ** jax.random.uniform(jax.random.fold_in(kz, 1), (), jnp.float32, -1.0, 2.0)
    layers = 2.0 ** jax.random.uniform(kl, (LAYERS, 1, 1), jnp.float32, -1.0, 1.0)
    x = together(ka, jax.random.normal(kx, shape, jnp.float32), much_x) * bump(kf, D, 4.0)
    dy = together(kb, jax.random.normal(kdy, shape, jnp.float32), much_dy)
    drawn = {"x": x.astype(jnp.bfloat16), "dy": (loud * dy * (SEQUENCES * TOKENS) ** -0.5).astype(jnp.bfloat16)}
    for key, name in zip(kw, NAMES, strict=True):
        w = jax.random.normal(key, SHAPES[name], jnp.float32) * SHAPES[name][1] ** -0.5
        drawn[name] = (w * {"w_gate": 1.0, "w_up": bump(kh, FF, 4.0), "w_down": layers}[name]).astype(jnp.bfloat16)
    for key, name in zip(km, NAMES, strict=True):
        drawn[f"m_{name}"] = 0.1 * jax.random.normal(key, SHAPES[name], jnp.float32)
    for key, name in zip(kv, NAMES, strict=True):
        drawn[f"v_{name}"] = jax.random.uniform(key, SHAPES[name], jnp.float32, 0.005, 0.015)
    return drawn


def matmul(a, w):
    return jnp.dot(a, w, preferred_element_type=jnp.float32).astype(jnp.bfloat16)


def normed(h):
    wide = h.astype(jnp.float32)
    scale = lax.rsqrt(jnp.mean(wide**2, -1, keepdims=True) + 1e-6)
    return (wide * scale).astype(jnp.bfloat16)


def layer(h, w):
    a = normed(h)
    gate = jnp.dot(a, w["w_gate"], preferred_element_type=jnp.float32)
    up = jnp.dot(a, w["w_up"], preferred_element_type=jnp.float32)
    return h + matmul((jax.nn.silu(gate) * up).astype(jnp.bfloat16), w["w_down"])


def adamw(w, m, v, g):
    m = 0.9 * m + 0.1 * g
    v = 0.95 * v + 0.05 * g * g
    step = m * lax.rsqrt(v + 1e-8) + 0.1 * w
    return (w - 0.02 * step).astype(jnp.bfloat16), m, v


def clipped(gradients, sum_of_squares, count):
    factor = jnp.minimum(1.0, 0.5 * lax.rsqrt(sum_of_squares / count + 1e-30))
    return [g * factor for g in gradients]


def stack(weights, h):
    return lax.scan(lambda h, w: (layer(h, w), None), h, weights)[0]


def reference(x, dy, w_gate, w_up, w_down, m_w_gate, m_w_up, m_w_down, v_w_gate, v_w_up, v_w_down):
    weights = dict(zip(NAMES, (w_gate, w_up, w_down), strict=True))

    def take(so_far, sequence):
        h, by_y = sequence
        _, back = jax.vjp(lambda w: stack(w, h), weights)
        return jax.tree.map(lambda total, term: total + term.astype(jnp.float32), so_far, back(by_y)[0]), None

    none_yet = {name: jnp.zeros(w.shape, jnp.float32) for name, w in weights.items()}
    by_weights, _ = lax.scan(take, none_yet, (x, dy))
    gradients = [by_weights[name].astype(jnp.bfloat16).astype(jnp.float32) for name in NAMES]
    gradients = clipped(gradients, sum(jnp.sum(g * g) for g in gradients), sum(g.size for g in gradients))
    new = [
        adamw(w.astype(jnp.float32), m, v, g)
        for w, m, v, g in zip((w_gate, w_up, w_down), (m_w_gate, m_w_up, m_w_down), (v_w_gate, v_w_up, v_w_down), gradients, strict=True)
    ]
    return tuple(one[which] for which in range(3) for one in new)
```

```python
import functools, math
import jax, jax.numpy as jnp
from jax import lax
from jax.experimental import pallas as pl
from jax.experimental.pallas import tpu as pltpu
from jax.sharding import PartitionSpec as P
MESH = pl.DeviceIdType.MESH
bf = jnp.bfloat16

class Place:
    def __init__(self, n):
        self.side = side = math.isqrt(n // 2)
        me = lax.axis_index("dp")
        self.c = c = lax.rem(me, 2)
        chip = me // 2
        x, y = chip // side, lax.rem(chip, side)
        self.i1 = x + c * (y - x)
        self.i2 = y + c * (x - y)
        self.m1 = side + c * (1 - side)
        self.m2 = 1 + c * (side - 1)
        self.partner = me + 1 - 2 * c
    def mod(self, a):
        return lax.rem(a + 2 * self.side, self.side)
    def chip(self, j1, j2):
        return j1 * self.m1 + j2 * self.m2
    def next1(self, d):
        return 2 * self.chip(self.mod(self.i1 + d), self.i2) + self.c
    def next2(self, d):
        return 2 * self.chip(self.i1, self.mod(self.i2 + d)) + self.c

def barrier(p):
    sem = pltpu.get_barrier_semaphore()
    others = [p.partner, p.next1(1), p.next1(-1), p.next2(1), p.next2(-1)]
    for o in others:
        pl.semaphore_signal(sem, inc=1, device_id={"dp": o}, device_id_type=MESH)
    pl.semaphore_wait(sem, len(others))

DIRS = (1, -1)

class Gather:
    STAGES = 8
    def __init__(self, p, own, block, group, sems):
        self.p, self.own, self.block, self.group = p, own, block, group
        self.local, self.s1, self.r1, self.s2, self.r2, self.sd, self.rd = sems
    def remote(self, src, dst, s, r, dev):
        return pltpu.make_async_remote_copy(src_ref=src, dst_ref=dst, send_sem=s, recv_sem=r, device_id={"dp": dev}, device_id_type=MESH)
    def c1(self, j, e, k):
        p, d = self.p, DIRS[e]
        here = self.block(j, e, p.mod(p.i1 - d * k), p.i2)
        return self.remote(self.own(j, e) if k == 0 else here, here, self.s1.at[j, e, k], self.r1.at[j, e, k], p.next1(d))
    def c2(self, j, e, k, core):
        p, d = self.p, DIRS[e]
        g = self.group(j, e, core, p.mod(p.i2 - d * k))
        return self.remote(g, g, self.s2.at[j, e, k], self.r2.at[j, e, k], p.next2(d))
    def cd(self, j, e, k, core):
        p, d = self.p, DIRS[e]
        g = self.group(j, e, core, p.mod(p.i2 - d * k))
        return self.remote(g, g, self.sd.at[j, e, k], self.rd.at[j, e, k], p.partner)
    def cl(self, j, e):
        p = self.p
        return pltpu.make_async_copy(self.own(j, e), self.block(j, e, p.i1, p.i2), self.local.at[j, e])
    def stage(self, k, j):
        p = self.p
        n = p.side
        if k == 0:
            for e in (0, 1):
                self.c1(j, e, 0).start()
                self.cl(j, e).start()
        elif k < n:
            for e in (0, 1):
                self.c1(j, e, k - 1).wait_recv()
                if k < n - 1:
                    self.c1(j, e, k).start()
            if k == n - 1:
                for e in (0, 1):
                    self.cl(j, e).wait()
                self.both(j, 0)
        elif k < 2 * n - 1:
            for e in (0, 1):
                self.c2(j, e, k - n, 0).wait_recv()
            self.both(j, k - n + 1)
        else:
            for e in (0, 1):
                for s in range(n):
                    self.cd(j, e, s, 0).wait_recv()
                    self.cd(j, e, s, 0).wait_send()
                for s in range(n - 1):
                    self.c1(j, e, s).wait_send()
                    self.c2(j, e, s, 0).wait_send()
    def both(self, j, k):
        for core in (0, 1):
            @pl.when(self.p.c == core)
            def _():
                for e in (0, 1):
                    if k < self.p.side - 1:
                        self.c2(j, e, k, core).start()
                    self.cd(j, e, k, core).start()

def gather_sems(n, side):
    D = pltpu.SemaphoreType.DMA
    return [D((n, 2)), D((n, 2, side - 1)), D((n, 2, side - 1)), D((n, 2, side - 1)), D((n, 2, side - 1)), D((n, 2, side)), D((n, 2, side))]

def gather_all(n, wg, wu, wd, lag=1, cg=256, cd=128, cid=1, order="gdg"):
    side = math.isqrt(n // 2)
    L, R, F = wg.shape
    Rd, Dm = wd.shape[1:]
    ng, nd = F // cg, Dm // (2 * cd)
    def kernel(wg_ref, wu_ref, wd_ref, og, ou, od, *sems):
        p = Place(n)
        barrier(p)
        def streams():
            out = []
            for l in range(L):
                def own(j, e, l=l):
                    return (wg_ref, wu_ref)[e].at[l, :, pl.ds(pl.multiple_of(j * cg, cg), cg)]
                def view(j, e, l=l):
                    return (og, ou)[e].at[l, :, :, :, :, pl.ds(pl.multiple_of(j * cg, cg), cg)]
                def own_d(j, e, l=l):
                    return wd_ref.at[l, :, pl.ds(pl.multiple_of((2 * j + e) * cd, cd), cd)]
                def view_d(j, e, l=l):
                    return od.at[l, :, :, :, :, pl.ds(pl.multiple_of((2 * j + e) * cd, cd), cd)]
                for own_, view_, m, s in ((own, view, ng, sems[14 * l:14 * l + 7]), (own_d, view_d, nd, sems[14 * l + 7:14 * l + 14])):
                    def block(j, e, j1, j2, view_=view_):
                        return view_(j, e).at[j1 + p.c * (j2 - j1), j2 + p.c * (j1 - j2), p.c]
                    def group(j, e, core, j2, view_=view_):
                        return view_(j, e).at[:, j2, 0] if core == 0 else view_(j, e).at[j2, :, 1]
                    out.append((Gather(p, own_, block, group, s), m))
            return out
        st = streams()
        if order == "gdg":
            st = [st[0], st[1], st[3], st[2]]
        starts, at = [], 0
        for g, m in st:
            starts.append(at); at += m
        total = at + (Gather.STAGES - 1) * lag
        def body(i, _):
            for k in reversed(range(Gather.STAGES)):
                for (g, m), lo in zip(st, starts):
                    j = i - lo - k * lag
                    @pl.when((j >= 0) & (j < m))
                    def _():
                        g.stage(k, j)
            return 0
        lax.fori_loop(0, total, body, 0)
    S = jax.ShapeDtypeStruct
    sems = []
    for l in range(L):
        sems += gather_sems(ng, side) + gather_sems(nd, side)
    V, A = pl.BlockSpec(memory_space=pltpu.VMEM), pl.BlockSpec(memory_space=pl.ANY)
    og, ou, od = pl.pallas_call(
        kernel, name="gather",
        out_shape=[S((L, side, side, 2, R, F), bf), S((L, side, side, 2, R, F), bf), S((L, side, side, 2, Rd, Dm), bf)],
        in_specs=[V] * 3, out_specs=[A] * 3, scratch_shapes=sems,
        compiler_params=pltpu.CompilerParams(collective_id=cid, has_side_effects=True, vmem_limit_bytes=48 * 2**20),
    )(wg, wu, wd)
    return og.reshape(L, n * R, F), ou.reshape(L, n * R, F), od.reshape(L, n * Rd, Dm)


f32 = jnp.float32

class Scatter:
    STAGES = 8
    def __init__(self, p, m, lag, bufs, done):
        self.p, self.m, self.lag, self.done = p, m, lag, done
        (self.own, self.q, self.snd1, self.rcv1, self.mid, self.snd2, self.rcv2,
         self.sd, self.rd, self.s1, self.r1, self.s2, self.r2) = bufs
        self.keep, self.pool = scatter_slots(m, lag)
    @staticmethod
    def remote(src, dst, s, r, dev):
        return pltpu.make_async_remote_copy(src_ref=src, dst_ref=dst, send_sem=s, recv_sem=r, device_id={"dp": dev}, device_id_type=MESH)
    def slot(self, j, h):
        mine, other = lax.rem(j, self.keep), self.keep + lax.rem(j, self.pool)
        return mine + (other - mine) * (self.p.c + h - 2 * self.p.c * h)
    def cd(self, j):
        return self.remote(self.own.at[self.keep + lax.rem(j, self.pool)], self.q.at[j], self.sd.at[j], self.rd.at[j], self.p.partner)
    def c1(self, j, e, k):
        return self.remote(self.snd1.at[lax.rem(j, self.snd1.shape[0]), e, k], self.rcv1.at[j, e, k], self.s1.at[j, e, k], self.r1.at[j, e, k], self.p.next1(DIRS[e]))
    def c2(self, j, e, k):
        return self.remote(self.snd2.at[lax.rem(j, self.snd2.shape[0]), e, k], self.rcv2.at[j, e, k], self.s2.at[j, e, k], self.r2.at[j, e, k], self.p.next2(DIRS[e]))
    def send(self, j):
        self.cd(j).start()
    def mine(self, j, e, j1, b):
        at = self.p.chip(j1, b)
        return self.own[lax.rem(j, self.keep), e, at].astype(f32) + self.q[j, e, at].astype(f32)
    def stage(self, k, j):
        p, n = self.p, self.p.side
        if k == 1:
            self.cd(j).wait_recv()
            self.cd(j).wait_send()
        elif k <= n:
            for e in (0, 1):
                self.c1(j, e, k - 2).wait_recv()
                self.c1(j, e, k - 2).wait_send()
        else:
            for e in (0, 1):
                self.c2(j, e, k - n - 1).wait_recv()
                self.c2(j, e, k - n - 1).wait_send()
        for e in (0, 1):
            d = DIRS[e]
            if k <= n:
                g = p.mod(p.i1 - d * k)
                for b in range(n):
                    v = self.mine(j, e, g, b)
                    if k > 1:
                        v = self.rcv1[j, e, k - 2, b].astype(f32) + v
                    if k < n:
                        self.snd1[lax.rem(j, self.snd1.shape[0]), e, k - 1, b] = v.astype(bf)
                    else:
                        self.mid[lax.rem(j, self.mid.shape[0]), e, b] = v
            if k >= n:
                v = self.mid[lax.rem(j, self.mid.shape[0]), e, p.mod(p.i2 - d * (k - n + 1))]
                if k > n:
                    v = self.rcv2[j, e, k - n - 1].astype(f32) + v
                if k < 2 * n - 1:
                    self.snd2[lax.rem(j, self.snd2.shape[0]), e, k - n] = v.astype(bf)
                else:
                    self.done(j, e, v)
        for e in (0, 1):
            if k < n:
                self.c1(j, e, k - 1).start()
            elif k < 2 * n - 1:
                self.c2(j, e, k - n).start()

def scatter_slots(m, lag):
    return min(m, 4 * lag), min(m, lag + 1)

def scatter_bufs(m, lag, side, R, C):
    keep, pool = scatter_slots(m, lag)
    few, V, D = min(m, lag + 1), pltpu.VMEM, pltpu.SemaphoreType.DMA
    return [V((keep + pool, 2, side * side, R, C), bf), V((m, 2, side * side, R, C), bf),
            V((few, 2, side - 1, side, R, C), bf), V((m, 2, side - 1, side, R, C), bf),
            V((min(m, 3 * lag + 1), 2, side, R, C), f32),
            V((few, 2, side - 1, R, C), bf), V((m, 2, side - 1, R, C), bf),
            D((m,)), D((m,)), D((m, 2, side - 1)), D((m, 2, side - 1)), D((m, 2, side - 1)), D((m, 2, side - 1))]

TN = (((0,), (0,)), ((), ()))

def grads(n, a, act, dgate, dup, dy, lag=2, lagd=1, cg=256, cd=128, cid=2):
    side = math.isqrt(n // 2)
    T, Dm = a.shape
    F = act.shape[1]
    R, Rd, ng, nd = Dm // n, F // n, F // cg, Dm // (2 * cd)
    half = F // 2
    chips = side * side
    def kernel(a_h, act_h, dg_h, du_h, dy_h, og, ou, od, a_v, act_v, dg_v, dy_v, ld, ldg, ldy, *bufs):
        p = Place(n)
        def load_act(m):
            cols = pl.ds(m * half, half)
            return pltpu.make_async_copy(act_h.at[:, cols], act_v.at[:, cols], ld.at[m])
        def load_a():
            return pltpu.make_async_copy(a_h, a_v, ld.at[2])
        def load_dy(j):
            return pltpu.make_async_copy(dy_h.at[:, pl.ds(pl.multiple_of(j * 2 * cd, 2 * cd), 2 * cd)], dy_v.at[lax.rem(j, 2)], ldy.at[lax.rem(j, 2)])
        def load_dg(j, e):
            return pltpu.make_async_copy((dg_h, du_h)[e].at[:, pl.ds(pl.multiple_of(j * cg, cg), cg)], dg_v.at[lax.rem(j, 2), e], ldg.at[lax.rem(j, 2), e])
        load_dy(0).start(); load_act(0).start(); load_act(1).start()
        barrier(p)
        def done_d(j, e, v):
            od[:, pl.ds(pl.multiple_of((2 * j + e) * cd, cd), cd)] = v.astype(bf)
        def done_g(j, e, v):
            (og, ou)[e][:, pl.ds(pl.multiple_of(j * cg, cg), cg)] = v.astype(bf)
        sd = Scatter(p, nd, lagd, bufs[:13], done_d)
        sg = Scatter(p, ng, lag, bufs[13:], done_g)
        load_dy(0).wait(); load_act(0).wait()
        def make_d(j):
            @pl.when(j + 1 < nd)
            def _(): load_dy(j + 1).start()
            @pl.when(j == 0)
            def _(): load_a().start()
            @pl.when(j == nd - 1)
            def _():
                for e in (0, 1): load_dg(0, e).start()
            for m in (0, 1):
                if m == 1:
                    @pl.when(j == 0)
                    def _(): load_act(1).wait()
                val = lax.dot_general(act_v[:, m * half:(m + 1) * half], dy_v[lax.rem(j, 2)], TN, preferred_element_type=f32)
                for e in (0, 1):
                    v = val[:, e * cd:(e + 1) * cd].reshape(chips // 2, 2, Rd, cd).astype(bf)
                    for h in (0, 1):
                        sd.own[sd.slot(j, h), e, m * chips // 2:(m + 1) * chips // 2] = v[:, h]
            sd.send(j)
            @pl.when(j + 1 < nd)
            def _(): load_dy(j + 1).wait()
        def make_g(j):
            @pl.when(j + 1 < ng)
            def _():
                for e in (0, 1): load_dg(j + 1, e).start()
            @pl.when(j == 0)
            def _(): load_a().wait()
            for e in (0, 1):
                load_dg(j, e).wait()
            for e in (0, 1):
                val = lax.dot_general(a_v[...], dg_v[lax.rem(j, 2), e], TN, preferred_element_type=f32)
                v = val.reshape(chips, 2, R, cg).astype(bf)
                for h in (0, 1):
                    sg.own[sg.slot(j, h), e] = v[:, h]
            sg.send(j)
        streams = ((sd, nd, 0, lagd, make_d), (sg, ng, nd, lag, make_g))
        total = max(lo + m + (Scatter.STAGES - 1) * lg for _, m, lo, lg, _ in streams)
        def body(i, _):
            for k in reversed(range(Scatter.STAGES)):
                for s, m, lo, lg, make in streams:
                    j = i - lo - k * lg
                    @pl.when((j >= 0) & (j < m))
                    def _():
                        make(j) if k == 0 else s.stage(k, j)
            return 0
        lax.fori_loop(0, total, body, 0)
    S, V, A, D = jax.ShapeDtypeStruct, pl.BlockSpec(memory_space=pltpu.VMEM), pl.BlockSpec(memory_space=pl.ANY), pltpu.SemaphoreType.DMA
    return pl.pallas_call(
        kernel, name="grads",
        out_shape=[S((R, F), bf), S((R, F), bf), S((Rd, Dm), bf)],
        in_specs=[A] * 5, out_specs=[V] * 3,
        scratch_shapes=[pltpu.VMEM((T, Dm), bf), pltpu.VMEM((T, F), bf), pltpu.VMEM((2, 2, T, cg), bf), pltpu.VMEM((2, T, 2 * cd), bf), D((3,)), D((2, 2)), D((2,)),
                        *scatter_bufs(nd, lagd, side, Rd, cd), *scatter_bufs(ng, lag, side, R, cg)],
        compiler_params=pltpu.CompilerParams(collective_id=cid, has_side_effects=True, vmem_limit_bytes=67043328),
    )(a, act, dgate, dup, dy)


def total(n, part, cid=9):
    def kernel(x_ref, o_ref, got, send, recv):
        me = lax.axis_index("dp")
        sem = pltpu.get_barrier_semaphore()
        def other(k):
            return lax.rem(me + k, n)
        def greet(k, _):
            pl.semaphore_signal(sem, inc=1, device_id={"dp": other(k)}, device_id_type=MESH)
            return 0
        lax.fori_loop(1, n, greet, 0)
        pl.semaphore_wait(sem, n - 1)
        def copy(k, slot):
            return pltpu.make_async_remote_copy(src_ref=x_ref, dst_ref=got.at[slot], send_sem=send.at[k], recv_sem=recv.at[slot], device_id={"dp": other(k)}, device_id_type=MESH)
        def start(k, _):
            copy(k, me).start()
            return 0
        lax.fori_loop(1, n, start, 0)
        got[me] = x_ref[...]
        def wait(k, _):
            copy(k, me).wait_send()
            copy(k, other(k)).wait_recv()
            return 0
        lax.fori_loop(1, n, wait, 0)
        o_ref[...] = jnp.sum(got[...], axis=0)
    V = pl.BlockSpec(memory_space=pltpu.VMEM)
    D = pltpu.SemaphoreType.DMA
    return pl.pallas_call(
        kernel, name="total", out_shape=jax.ShapeDtypeStruct(part.shape, jnp.float32), in_specs=[V], out_specs=V,
        scratch_shapes=[pltpu.VMEM((n, *part.shape), jnp.float32), D((n,)), D((n,))],
        compiler_params=pltpu.CompilerParams(collective_id=cid, has_side_effects=True),
    )(part)


def matmul(a, w):
    return jnp.dot(a, w, preferred_element_type=f32).astype(bf)


def matmul_t(a, w):
    return lax.dot_general(a, w, (((1,), (1,)), ((), ())), preferred_element_type=f32).astype(bf)


def normed(h):
    wide = h.astype(f32)
    scale = lax.rsqrt(jnp.mean(wide**2, -1, keepdims=True) + 1e-6)
    return (wide * scale).astype(bf)


def gated(gate, up):
    return (jax.nn.silu(gate) * up).astype(bf)


def adamw(w, m, v, g):
    m = 0.9 * m + 0.1 * g
    v = 0.95 * v + 0.05 * g * g
    step = m * lax.rsqrt(v + 1e-8) + 0.1 * w
    return (w - 0.02 * step).astype(bf), m, v


def clipped(gradients, sum_of_squares, count):
    factor = jnp.minimum(1.0, 0.5 * lax.rsqrt(sum_of_squares / count + 1e-30))
    return [g * factor for g in gradients]


def solution(mesh):
    n = mesh.shape["dp"]

    def step(x, dy, *arrays):
        weights, m, v = (arrays[i : i + 3] for i in (0, 3, 6))
        layers = weights[0].shape[0]
        wg, wu, wd = gather_all(n, *weights, lag=4, cd=256)
        h, kept = x[0], []
        for l in range(layers):
            a = normed(h)
            gate = jnp.dot(a, wg[l], preferred_element_type=f32)
            up = jnp.dot(a, wu[l], preferred_element_type=f32)
            act, back = jax.vjp(gated, gate, up)
            kept.append((h, a, act, back))
            if l < layers - 1:
                h = h + matmul(act, wd[l])
        by_h, mine = dy[0], [None] * layers
        for l in reversed(range(layers)):
            h, a, act, back = kept[l]
            dgate, dup = (d.astype(bf) for d in back(matmul_t(by_h, wd[l])))
            mine[l] = grads(n, a, act, dgate, dup, by_h, cid=2 + l)
            if l:
                da = matmul_t(dgate, wg[l]) + matmul_t(dup, wu[l])
                by_h = by_h + jax.vjp(normed, h)[1](da)[0]
        gradients = [jnp.stack([mine[l][i] for l in range(layers)]).astype(f32) for i in range(3)]
        part = sum(jnp.sum(g * g) for g in gradients)
        squares = total(n, jnp.broadcast_to(part / 1024, (8, 128)))
        squares = jnp.sum(squares)
        gradients = clipped(gradients, squares, n * sum(g.size for g in gradients))
        new = [adamw(w.astype(f32), m, v, g) for w, m, v, g in zip(weights, m, v, gradients, strict=True)]
        return tuple(one[which] for which in range(3) for one in new)

    states, cut = P(("rep", "dp"), None, None), P(None, "dp", None)
    return jax.shard_map(
        step,
        mesh=mesh,
        in_specs=(states, states) + (cut,) * 9,
        out_specs=(P("rep", "dp", None),) * 9,
        check_vma=False,
    )
```

```python
import functools, math
import jax, jax.numpy as jnp
from jax import lax
from jax.experimental import pallas as pl
from jax.experimental.pallas import tpu as pltpu
from jax.sharding import PartitionSpec as P
MESH = pl.DeviceIdType.MESH
bf = jnp.bfloat16

class Place:
    def __init__(self, n):
        self.side = side = math.isqrt(n // 2)
        me = lax.axis_index("dp")
        self.c = c = lax.rem(me, 2)
        chip = me // 2
        x, y = chip // side, lax.rem(chip, side)
        self.i1 = x + c * (y - x)
        self.i2 = y + c * (x - y)
        self.m1 = side + c * (1 - side)
        self.m2 = 1 + c * (side - 1)
        self.partner = me + 1 - 2 * c
    def mod(self, a):
        return lax.rem(a + 2 * self.side, self.side)
    def chip(self, j1, j2):
        return j1 * self.m1 + j2 * self.m2
    def next1(self, d):
        return 2 * self.chip(self.mod(self.i1 + d), self.i2) + self.c
    def next2(self, d):
        return 2 * self.chip(self.i1, self.mod(self.i2 + d)) + self.c

def barrier(p):
    sem = pltpu.get_barrier_semaphore()
    others = [p.partner, p.next1(1), p.next1(-1), p.next2(1), p.next2(-1)]
    for o in others:
        pl.semaphore_signal(sem, inc=1, device_id={"dp": o}, device_id_type=MESH)
    pl.semaphore_wait(sem, len(others))

DIRS = (1, -1)
BOTH = (0, 1)

class Gather:
    STAGES = 6

    def __init__(self, p, own, block, row, core, sent, local, sems):
        self.p, self.own, self.block, self.row, self.core, self.sent, self.local = p, own, block, row, core, sent, local
        self.sl, self.s, self.sd, self.r, self.rd = sems

    def remote(self, src, dst, s, r, dev):
        return pltpu.make_async_remote_copy(src_ref=src, dst_ref=dst, send_sem=s, recv_sem=r, device_id={"dp": dev}, device_id_type=MESH)

    def copy(self, k, j, e, core=0):
        p, d = self.p, DIRS[e]
        if k < 2:
            here = self.block(j, e, p.mod(p.i1 - d), p.i2) if k else self.block(j, None, p.i1, p.i2)
            src, to = here if k else self.own(j), p.next1(d)
        else:
            src = here = self.row(j, e, core, p.mod(p.i2 - d)) if k == 3 else self.row(j, None, core, p.i2)
            to = p.next2(d)
        return self.remote(src, here, self.s.at[k, e], self.r.at[j, k, e], to)

    def across(self, j, core):
        g = self.core(j, core)
        return self.remote(g, g, self.sd, self.rd.at[j], self.p.partner)

    def copies(self):
        return [pltpu.make_async_copy(a, b, self.sl.at[k]) for k, (a, b) in enumerate(self.local)]

    def begin(self):
        for c in self.copies():
            c.start()

    def stage(self, k, j):
        if k == self.STAGES - 1:
            self.across(j, 1 - self.p.c).wait_recv()
            return
        if k:
            for e in BOTH:
                self.copy(k - 1, j, e).wait_recv()
        if k < 2:
            for e in BOTH:
                self.copy(k, j, e).start()
        elif k < 4:
            if k == 2:
                @pl.when(j == 0)
                def _():
                    for c in self.copies():
                        c.wait()
            for core in BOTH:
                @pl.when(self.p.c == core)
                def _():
                    for e in BOTH:
                        self.copy(k, j, e, core).start()
        else:
            self.across(j, self.p.c).start()

    def end(self):
        *kinds, across = self.sent
        for k, view in enumerate(kinds):
            for e in BOTH:
                pltpu.make_async_copy(view, view, self.s.at[k, e]).wait()
        pltpu.make_async_copy(across, across, self.sd).wait()


def gather_sems(m, local):
    D = pltpu.SemaphoreType.DMA
    return [D((local,)), D((4, 2)), D, D((m, 4, 2)), D((m,))]


f32 = jnp.float32
TN = (((0,), (0,)), ((), ()))
NT = (((1,), (1,)), ((), ()))


class Scatter:
    STAGES = 6

    def __init__(self, p, lag, bufs, done):
        self.p, self.done = p, done
        self.own, self.q, self.mid, *self.bufs, self.sd, self.rd, self.s, self.r = bufs
        self.keep, self.pool = scatter_slots(self.q.shape[0], lag)

    def remote(self, src, dst, s, r, dev):
        return pltpu.make_async_remote_copy(src_ref=src, dst_ref=dst, send_sem=s, recv_sem=r, device_id={"dp": dev}, device_id_type=MESH)

    def slot(self, j, h):
        mine, other = lax.rem(j, self.keep), self.keep + lax.rem(j, self.pool)
        return mine + (other - mine) * (self.p.c + h - 2 * self.p.c * h)

    def across(self, j):
        return self.remote(self.own.at[self.keep + lax.rem(j, self.pool)], self.q.at[j], self.sd.at[j], self.rd.at[j], self.p.partner)

    def out(self, k):
        return self.bufs[2 * k]

    def got(self, k):
        return self.bufs[2 * k + 1]

    def at(self, j, ref):
        return lax.rem(j, ref.shape[0])

    def copy(self, k, j, e):
        to = self.p.next1(DIRS[e]) if k < 2 else self.p.next2(DIRS[e])
        return self.remote(self.out(k).at[self.at(j, self.out(k)), e], self.got(k).at[j, e], self.s.at[j, k, e], self.r.at[j, k, e], to)

    def send(self, j):
        self.across(j).start()

    def mine(self, j, e, j1, b):
        at = self.p.chip(j1, b)
        return self.own[lax.rem(j, self.keep), e, at].astype(f32) + self.q[j, e, at].astype(f32)

    def stage(self, k, j):
        p, n = self.p, self.p.side
        for c in [self.across(j)] if k == 1 else [self.copy(k - 2, j, e) for e in BOTH]:
            c.wait_recv()
            c.wait_send()
        m = self.at(j, self.mid)
        if k < 5:
            o, out = self.out(k - 1), self.at(j, self.out(k - 1))
        if k == 1:
            for e in BOTH:
                for b in range(n):
                    o[out, e, 0, b] = self.mine(j, e, p.mod(p.i1 + 2), b).astype(bf)
                    o[out, e, 1, b] = self.mine(j, 1 - e, p.mod(p.i1 + DIRS[e]), b).astype(bf)
        elif k == 2:
            for e in BOTH:
                for b in range(n):
                    o[out, e, b] = (self.got(0)[j, e, 0, b].astype(f32) + self.mine(j, e, p.mod(p.i1 + DIRS[e]), b)).astype(bf)
        elif k == 3:
            for h in BOTH:
                for b in range(n):
                    self.mid[m, h, b] = self.got(1)[j, h, b].astype(f32) + self.got(0)[j, 1 - h, 1, b].astype(f32) + self.mine(j, h, p.i1, b)
            for e in BOTH:
                o[out, e, 0] = self.mid[m, e, p.mod(p.i2 + 2)].astype(bf)
                o[out, e, 1] = self.mid[m, 1 - e, p.mod(p.i2 + DIRS[e])].astype(bf)
        elif k == 4:
            for e in BOTH:
                o[out, e] = (self.got(2)[j, e, 0].astype(f32) + self.mid[m, e, p.mod(p.i2 + DIRS[e])]).astype(bf)
        else:
            for h in BOTH:
                self.done(j, h, self.got(3)[j, h].astype(f32) + self.got(2)[j, 1 - h, 1].astype(f32) + self.mid[m, h, p.i2])
        if k < 5:
            for e in BOTH:
                self.copy(k - 1, j, e).start()


def scatter_slots(m, lag):
    return min(m, 3 * lag), min(m, lag + 1)


def scatter_bufs(m, lag, side, R, C):
    keep, pool = scatter_slots(m, lag)
    few, V, D = min(m, lag + 1), pltpu.VMEM, pltpu.SemaphoreType.DMA
    pairs = [V((k, 2, *s, R, C), bf) for s in ((2, side), (side,), (2,), ()) for k in (few, m)]
    return [V((keep + pool, 2, side * side, R, C), bf), V((m, 2, side * side, R, C), bf), V((min(m, 2 * lag + 1), 2, side, R, C), f32), *pairs,
            D((m,)), D((m,)), D((m, 4, 2)), D((m, 4, 2))]


def normed_rows(h):
    wide = h.astype(f32)
    scale = lax.rsqrt(jnp.mean(wide * wide, -1, keepdims=True) + 1e-6)
    return (wide * scale).astype(bf)


def forward(n, x, dy, wg, wu, wd, lag=3, cg=256, cd=128, cid=1):
    side = math.isqrt(n // 2)
    T, Dm = x.shape
    L, R, F = wg.shape
    Rd = wd.shape[1]
    ng, nd, rows, tile = F // cg, Dm // (2 * cd), T // 2, T // 8
    width = 2 * cd

    def kernel(x_h, dy_h, wg_ref, wu_ref, wd_ref, ogu, od, g0, u0, act0, h1, a0, a1, act1, dg1, du1,
               xv, av, dyv, actv, own_v, wb, wdb, wdr, stg, st3, s_in, s_w, s_wd, s_wr, s_stg, s_act, s_out, s_st3, *sems):
        p = Place(n)
        pltpu.make_async_copy(x_h, xv, s_in.at[0]).start()
        pltpu.make_async_copy(dy_h, dyv, s_in.at[1]).start()
        own_v[:, 0] = wg_ref[...]
        own_v[:, 1] = wu_ref[...]
        barrier(p)
        every = slice(None)

        def cols(j, w):
            return pl.ds(pl.multiple_of(j * w, w), w)
        def core_rows(c):
            return pl.ds(c * Rd if isinstance(c, int) else pl.multiple_of(c * Rd, 8), Rd)
        def place(q, m):
            return q // m, lax.rem(q, m)

        def at_g(q, e, x, y, c):
            l, j = place(q, ng)
            return ogu.at[l, x, y, c, every if e is None else e, every, cols(j, cg)]
        def at_d(q, e, x, y, c):
            l, j = place(q, nd)
            return od.at[l, x, y, core_rows(c), cols(j, width) if e is None else cols(2 * j + e, cd)]
        def own_g(q):
            l, j = place(q, ng)
            return own_v.at[l, every, every, cols(j, cg)]
        def own_d(q):
            l, j = place(q, nd)
            return wd_ref.at[l, every, cols(j, width)]

        def stream(at, own, sent, local, sems):
            x, y = p.i1 + p.c * (p.i2 - p.i1), p.i2 + p.c * (p.i1 - p.i2)
            def block(q, e, j1, j2):
                return at(q, e, j1 + p.c * (j2 - j1), j2 + p.c * (j1 - j2), p.c)
            def row(q, e, core, j2):
                return at(q, e, j2, every, core) if core else at(q, e, every, j2, core)
            def core(q, c):
                return at(q, None, every, every, c)
            return Gather(p, own, block, row, core, sent, local(x, y), sems)

        r0, h0 = core_rows(0), pl.ds(0, Dm // 2)
        sent_g = [ogu.at[:, 0, 0, 0], ogu.at[:, 0, 0, 0, 0], ogu.at[:, :, 0, 0], ogu.at[:, :, 0, 0, 0], ogu.at[:, :, :, 0]]
        sent_d = [od.at[:, 0, 0, r0], od.at[:, 0, 0, r0, h0], od.at[:, :, 0, r0], od.at[:, :, 0, r0, h0], od.at[:, :, :, r0]]
        G = stream(at_g, own_g, sent_g, lambda x, y: [(own_v.at[l], ogu.at[l, x, y, p.c]) for l in range(L)], sems[:5])
        Ds = stream(at_d, own_d, sent_d, lambda x, y: [(wd_ref.at[l], od.at[l, x, y, core_rows(p.c)]) for l in range(L)], sems[5:])
        G.begin()
        Ds.begin()
        downs = 2 * nd
        chunks, depth = 2 * ng + downs, (Gather.STAGES - 1) * lag

        def load_g(q):
            l, j = place(q, ng)
            return pltpu.make_async_copy(ogu.at[l, :, :, :, :, :, cols(j, cg)], wb.at[lax.rem(q, 2)], s_w.at[lax.rem(q, 2)])
        def load_d(j):
            return pltpu.make_async_copy(od.at[0, :, :, :, cols(j, width)], wdb.at[lax.rem(j, 2)], s_wd.at[lax.rem(j, 2)])
        def load_r(k):
            return pltpu.make_async_copy(od.at[1, k // side, lax.rem(k, side)], wdr.at[pl.ds(pl.multiple_of(k * 2 * Rd, 2 * Rd), 2 * Rd)], s_wr.at[k])
        def weights(q, e):
            return wb[lax.rem(q, 2), :, :, :, e].reshape(Dm, cg)
        def part(r):
            return pl.ds(pl.multiple_of(r * rows, rows), rows)
        def put_g(j, r):
            return [pltpu.make_async_copy(stg.at[r, e], (g0, u0)[e].at[part(r), cols(j, cg)], s_stg.at[r, e]) for e in BOTH]
        def put_act(j):
            return pltpu.make_async_copy(actv.at[:, cols(j, cg)], act0.at[:, cols(j, cg)], s_act.at[j])
        def put_3(j, r):
            return [pltpu.make_async_copy(st3.at[r, e], (act1, dg1, du1)[e].at[part(r), cols(j, cg)], s_st3.at[r, e]) for e in (0, 1, 2)]
        put_a0 = pltpu.make_async_copy(av, a0, s_out.at[0])
        put_h1 = pltpu.make_async_copy(xv, h1, s_out.at[1])
        put_a1 = pltpu.make_async_copy(av, a1, s_out.at[2])

        def norm():
            def one(r, _):
                rs_ = pl.ds(pl.multiple_of(r * tile, tile), tile)
                av[rs_, :] = normed_rows(xv[rs_, :])
                return 0
            lax.fori_loop(0, T // tile, one, 0)

        def first():
            pltpu.make_async_copy(x_h, xv, s_in.at[0]).wait()
            pltpu.make_async_copy(dy_h, dyv, s_in.at[1]).wait()
            norm()
            put_a0.start()

        def gate_up(j):
            load_g(j).wait()
            def one(r, _):
                @pl.when(j > 0)
                def _():
                    for c in put_g(j - 1, r):
                        c.wait()
                a = av[part(r), :]
                g = jnp.dot(a, weights(j, 0), preferred_element_type=f32)
                u = jnp.dot(a, weights(j, 1), preferred_element_type=f32)
                stg[r, 0] = g
                stg[r, 1] = u
                actv[part(r), cols(j, cg)] = (g * jax.nn.sigmoid(g) * u).astype(bf)
                for c in put_g(j, r):
                    c.start()
                return 0
            lax.fori_loop(0, 2, one, 0)
            put_act(j).start()

        def down(j):
            load_d(j).wait()
            def one(r, _):
                y = jnp.dot(actv[part(r), :], wdb[lax.rem(j, 2)].reshape(F, width), preferred_element_type=f32).astype(bf)
                xv[part(r), cols(j, width)] = xv[part(r), cols(j, width)] + y
                return 0
            lax.fori_loop(0, 2, one, 0)

        def second():
            for r in BOTH:
                for c in put_g(ng - 1, r):
                    c.wait()
            put_a0.wait()
            put_h1.start()
            norm()
            put_a1.start()

        def gate_up_back(j):
            load_g(ng + j).wait()
            @pl.when(j == 0)
            def _():
                def wait(k, _):
                    load_r(k).wait()
                    return 0
                lax.fori_loop(0, side * side, wait, 0)
            def one(r, _):
                @pl.when(j > 0)
                def _():
                    for c in put_3(j - 1, r):
                        c.wait()
                a = av[part(r), :]
                g = jnp.dot(a, weights(ng + j, 0), preferred_element_type=f32)
                u = jnp.dot(a, weights(ng + j, 1), preferred_element_type=f32)
                d = lax.dot_general(dyv[part(r), :], wdr[cols(j, cg), :], NT, preferred_element_type=f32).astype(bf).astype(f32)
                s = jax.nn.sigmoid(g)
                gs = g * s
                st3[r, 0] = (gs * u).astype(bf)
                st3[r, 1] = (d * u * (s + gs * (1.0 - s))).astype(bf)
                st3[r, 2] = (d * gs).astype(bf)
                for c in put_3(j, r):
                    c.start()
                return 0
            lax.fori_loop(0, 2, one, 0)

        def tick(t, _):
            for k in reversed(range(Gather.STAGES)):
                q = t - k * lag
                late = q >= ng + downs
                @pl.when((q >= 0) & (q < chunks) & ((q < ng) | late))
                def _():
                    j = q - jnp.where(late, downs, 0)
                    G.stage(k, j)
                    if k == Gather.STAGES - 1:
                        load_g(j).start()
                @pl.when((q >= ng) & (q < ng + downs))
                def _():
                    j = q - ng
                    Ds.stage(k, j)
                    if k == Gather.STAGES - 1:
                        @pl.when(j < nd)
                        def _():
                            load_d(j).start()
                        @pl.when(j == downs - 1)
                        def _():
                            def start(k, _):
                                load_r(k).start()
                                return 0
                            lax.fori_loop(0, side * side, start, 0)
            @pl.when(t == min(2, lag - 1))
            def _():
                first()
            m = t - depth - 1
            @pl.when((m >= 0) & (m < ng))
            def _():
                gate_up(m)
            @pl.when((m >= ng) & (m < ng + nd))
            def _():
                down(m - ng)
            @pl.when(m == ng + nd)
            def _():
                second()
            @pl.when(m >= ng + downs)
            def _():
                gate_up_back(m - ng - downs)
            return 0
        lax.fori_loop(0, chunks + depth + 1, tick, 0)
        for r in BOTH:
            for c in put_3(ng - 1, r):
                c.wait()
        G.end()
        Ds.end()
        def last(j, _):
            put_act(j).wait()
            return 0
        lax.fori_loop(0, ng, last, 0)
        put_h1.wait()
        put_a1.wait()

    S, V, A, D = jax.ShapeDtypeStruct, pl.BlockSpec(memory_space=pltpu.VMEM), pl.BlockSpec(memory_space=pl.ANY), pltpu.SemaphoreType.DMA
    VM = pltpu.VMEM
    sems = gather_sems(L * ng, L) + gather_sems(L * nd, L)
    wide, thin = S((T, F), bf), S((T, Dm), bf)
    out = pl.pallas_call(
        kernel, name="forward",
        out_shape=[S((L, side, side, 2, 2, R, F), bf), S((L, side, side, 2 * Rd, Dm), bf),
                   S((T, F), f32), S((T, F), f32), wide, thin, thin, thin, wide, wide, wide],
        in_specs=[A, A, V, V, V], out_specs=[A] * 11,
        scratch_shapes=[VM((T, Dm), bf), VM((T, Dm), bf), VM((T, Dm), bf), VM((T, F), bf), VM((L, 2, R, F), bf), VM((2, side, side, 2, 2, R, cg), bf), VM((2, side, side, 2 * Rd, width), bf), VM((F, Dm), bf),
                        VM((2, 2, rows, cg), f32), VM((2, 3, rows, cg), bf),
                        D((2,)), D((2,)), D((2,)), D((side * side,)), D((2, 2)), D((ng,)), D((3,)), D((2, 3)), *sems],
        compiler_params=pltpu.CompilerParams(collective_id=cid, has_side_effects=True, vmem_limit_bytes=67043328),
    )(x, dy, wg, wu, wd)
    ogu, od, *rest = out
    return ogu, od.reshape(L, n * Rd, Dm), *rest


class Layer:
    def __init__(self, n, a, act, lag, lagd, cg, cd):
        self.n, self.side = n, math.isqrt(n // 2)
        self.T, self.Dm = a.shape
        self.F = act.shape[1]
        self.R, self.Rd, self.ng, self.nd = self.Dm // n, self.F // n, self.F // cg, self.Dm // (2 * cd)
        self.lag, self.lagd, self.cg, self.cd, self.half, self.chips = lag, lagd, cg, cd, self.F // 2, self.side * self.side
    def bufs(self):
        return [*scatter_bufs(self.nd, self.lagd, self.side, self.Rd, self.cd), *scatter_bufs(self.ng, self.lag, self.side, self.R, self.cg)]
    def outs(self):
        S = jax.ShapeDtypeStruct
        return [S((self.R, self.F), bf), S((self.R, self.F), bf), S((self.Rd, self.Dm), bf), S((8, 128), f32)]
    def streams(self, p, og, ou, od, sq, bufs):
        def add(v):
            w = v.astype(f32)
            w = jnp.sum((w * w).reshape(w.shape[0] // 8, 8, w.shape[1]), 0)
            for k in range(w.shape[1] // 128):
                sq[...] += w[:, 128 * k:128 * k + 128]
        def done_d(j, e, v):
            v = v.astype(bf)
            od[:, pl.ds(pl.multiple_of((2 * j + e) * self.cd, self.cd), self.cd)] = v
            add(v)
        def done_g(j, e, v):
            v = v.astype(bf)
            (og, ou)[e][:, pl.ds(pl.multiple_of(j * self.cg, self.cg), self.cg)] = v
            add(v)
        sq[...] = jnp.zeros_like(sq)
        self.p = p
        split = len(bufs) // 2
        self.sd = Scatter(p, self.lagd, bufs[:split], done_d)
        self.sg = Scatter(p, self.lag, bufs[split:], done_g)
    def put_d(self, j, m, val):
        for e in BOTH:
            v = val[:, e * self.cd:(e + 1) * self.cd].reshape(self.chips // 2, 2, self.Rd, self.cd).astype(bf)
            for h in BOTH:
                self.sd.own[self.sd.slot(j, h), e, m * self.chips // 2:(m + 1) * self.chips // 2] = v[:, h]
    def put_g(self, j, val):
        for e in BOTH:
            v = val[:, e * self.cg:(e + 1) * self.cg].reshape(self.chips, 2, self.R, self.cg).astype(bf)
            for h in BOTH:
                self.sg.own[self.sg.slot(j, h), e] = v[:, h]
    def run(self, make_d, make_g, extra=0, more=None):
        streams = ((self.sd, self.nd, 0, self.lagd, make_d), (self.sg, self.ng, self.nd, self.lag, make_g))
        total = max(lo + m + (Scatter.STAGES - 1) * lg for _, m, lo, lg, _ in streams)
        total = max(total, self.nd + self.ng + extra)
        def body(i, _):
            for k in reversed(range(Scatter.STAGES)):
                for s, m, lo, lg, make in streams:
                    j = i - lo - k * lg
                    @pl.when((j >= 0) & (j < m))
                    def _():
                        make(j) if k == 0 else s.stage(k, j)
            if extra:
                j = i - self.nd - self.ng
                @pl.when((j >= 0) & (j < extra))
                def _():
                    more(j)
            return 0
        lax.fori_loop(0, total, body, 0)


def cols_of(j, w):
    return pl.ds(pl.multiple_of(j * w, w), w)


def backward_last(n, a, act, dgate, dup, dy, h, wgu, layer, lag=2, lagd=2, cg=256, cd=128, cid=2):
    k = Layer(n, a, act, lag, lagd, cg, cd)
    T, Dm, F, tile = k.T, k.Dm, k.F, k.T // 8
    def kernel(a_h, act_h, dg_h, du_h, dy_h, h_h, w_h, og, ou, od, sq, dh_h,
               a_v, act_v, dg_v, dy_v, row_v, h_v, y_v, o_v, ld, ldg, ldy, ldr, ldo, ldw, *bufs):
        p = Place(n)
        def load_act(m):
            cols = pl.ds(m * k.half, k.half)
            return pltpu.make_async_copy(act_h.at[:, cols], act_v.at[:T, cols], ld.at[m])
        load_a = pltpu.make_async_copy(a_h, a_v, ld.at[2])
        def load_dy(j):
            return pltpu.make_async_copy(dy_h.at[:, cols_of(j, 2 * cd)], dy_v.at[lax.rem(j, 2)], ldy.at[lax.rem(j, 2)])
        def load_dg(j, e):
            return pltpu.make_async_copy((dg_h, du_h)[e].at[:, cols_of(j, cg)], dg_v.at[lax.rem(j, 2), :, e * cg:(e + 1) * cg], ldg.at[lax.rem(j, 2), e])
        def load_w(d):
            for e in BOTH:
                chip = d // 2
                rows = pl.ds(pl.multiple_of((e * n + d) * k.R, k.R), k.R)
                pltpu.make_async_copy(w_h.at[layer, chip // k.side, lax.rem(chip, k.side), lax.rem(d, 2), e], act_v.at[rows], ldw).start()
            return 0
        w_v = act_v.at[:2 * Dm]
        def load_row(r, e):
            return pltpu.make_async_copy((dg_h, du_h)[e].at[cols_of(r, tile), :], row_v.at[e], ldr.at[e])
        def load_h(r):
            return pltpu.make_async_copy(h_h.at[cols_of(r, tile), :], h_v, ldr.at[2])
        def load_y(r):
            return pltpu.make_async_copy(dy_h.at[cols_of(r, tile), :], y_v, ldr.at[3])
        def put(r):
            return pltpu.make_async_copy(o_v, dh_h.at[cols_of(r, tile), :], ldo)
        load_dy(0).start(); load_act(0).start(); load_act(1).start()
        barrier(p)
        k.streams(p, og, ou, od, sq, bufs)
        load_dy(0).wait(); load_act(0).wait()
        def make_d(j):
            @pl.when(j + 1 < k.nd)
            def _(): load_dy(j + 1).start()
            @pl.when(j == 0)
            def _(): load_a.start()
            @pl.when(j == k.nd - 1)
            def _():
                for e in BOTH: load_dg(0, e).start()
            for m in BOTH:
                if m == 1:
                    @pl.when(j == 0)
                    def _(): load_act(1).wait()
                k.put_d(j, m, lax.dot_general(act_v[:T, m * k.half:(m + 1) * k.half], dy_v[lax.rem(j, 2)], TN, preferred_element_type=f32))
            k.sd.send(j)
            @pl.when(j + 1 < k.nd)
            def _(): load_dy(j + 1).wait()
        def make_g(j):
            @pl.when(j + 1 < k.ng)
            def _():
                for e in BOTH: load_dg(j + 1, e).start()
            @pl.when(j == 0)
            def _():
                lax.fori_loop(0, n, lambda d, _: load_w(d), 0)
                load_a.wait()
            @pl.when(j == k.ng - 1)
            def _():
                for e in BOTH: load_row(0, e).start()
                load_h(0).start(); load_y(0).start()
            for e in BOTH:
                load_dg(j, e).wait()
            k.put_g(j, lax.dot_general(a_v[...], dg_v[lax.rem(j, 2)], TN, preferred_element_type=f32))
            k.sg.send(j)
        def rows(r):
            @pl.when(r == 0)
            def _():
                pltpu.make_async_copy(w_v, w_v, ldw).wait()
            @pl.when(r > 0)
            def _():
                put(r - 1).wait()
            def again(c):
                @pl.when(r + 1 < T // tile)
                def _(): c.start()
            both = []
            for e in BOTH:
                load_row(r, e).wait()
                both.append(lax.dot_general(row_v[e], act_v[e * Dm:(e + 1) * Dm], NT, preferred_element_type=f32).astype(bf))
                again(load_row(r + 1, e))
            da = (both[0] + both[1]).astype(f32)
            load_h(r).wait(); load_y(r).wait()
            wide = h_v[...].astype(f32)
            s = lax.rsqrt(jnp.mean(wide * wide, -1, keepdims=True) + 1e-6)
            t = jnp.sum(da * wide, -1, keepdims=True) * (s * s * s) * (1.0 / Dm)
            o_v[...] = (da * s - wide * t).astype(bf) + y_v[...]
            put(r).start()
            again(load_h(r + 1)); again(load_y(r + 1))
        k.run(make_d, make_g, T // tile, rows)
        put(T // tile - 1).wait()
    V, A, D, VM = pl.BlockSpec(memory_space=pltpu.VMEM), pl.BlockSpec(memory_space=pl.ANY), pltpu.SemaphoreType.DMA, pltpu.VMEM
    return pl.pallas_call(
        kernel, name="backward_last", out_shape=[*k.outs(), jax.ShapeDtypeStruct((T, Dm), bf)], in_specs=[A] * 7, out_specs=[V] * 4 + [A],
        scratch_shapes=[VM((T, Dm), bf), VM((max(T, 2 * Dm), F), bf), VM((2, T, 2 * cg), bf), VM((2, T, 2 * cd), bf), VM((2, tile, F), bf), VM((tile, Dm), bf), VM((tile, Dm), bf), VM((tile, Dm), bf),
                        D((3,)), D((2, 2)), D((2,)), D((4,)), D, D, *k.bufs()],
        compiler_params=pltpu.CompilerParams(collective_id=cid, has_side_effects=True, vmem_limit_bytes=67043328),
    )(a, act, dgate, dup, dy, h, wgu)


def backward_first(n, a, act, gate, up, dh, wd, layer, lag=2, lagd=2, cg=256, cd=128, cid=3):
    k = Layer(n, a, act, lag, lagd, cg, cd)
    T, Dm, F, rows = k.T, k.Dm, k.F, k.T // 2
    def kernel(a_h, act_h, g_h, u_h, dh_h, wd_h, og, ou, od, sq, a_v, act_v, gu_v, dg_v, dh_v, wd_v, ld, ldg, ldw, *bufs):
        p = Place(n)
        def load_act(m):
            cols = pl.ds(m * k.half, k.half)
            return pltpu.make_async_copy(act_h.at[:, cols], act_v.at[:, cols], ld.at[m])
        load_a = pltpu.make_async_copy(a_h, a_v, ld.at[2])
        load_dh = pltpu.make_async_copy(dh_h, dh_v, ld.at[3])
        def part(r):
            return pl.ds(pl.multiple_of(r * rows, rows), rows)
        def load_gu(j, r):
            return [pltpu.make_async_copy((g_h, u_h)[e].at[part(r), cols_of(j, cg)], gu_v.at[r, e], ldg.at[r, e]) for e in BOTH]
        def load_wd(j):
            return pltpu.make_async_copy(wd_h.at[layer, cols_of(j, cg), :], wd_v, ldw)
        load_dh.start(); load_act(0).start(); load_act(1).start()
        barrier(p)
        k.streams(p, og, ou, od, sq, bufs)
        load_dh.wait(); load_act(0).wait()
        def make_d(j):
            @pl.when(j == 0)
            def _(): load_a.start()
            @pl.when(j == k.nd - 1)
            def _():
                for r in BOTH:
                    for c in load_gu(0, r): c.start()
                load_wd(0).start()
            for m in BOTH:
                if m == 1:
                    @pl.when(j == 0)
                    def _(): load_act(1).wait()
                k.put_d(j, m, lax.dot_general(act_v[:, m * k.half:(m + 1) * k.half], dh_v[:, cols_of(j, 2 * cd)], TN, preferred_element_type=f32))
            k.sd.send(j)
        def make_g(j):
            @pl.when(j == 0)
            def _(): load_a.wait()
            load_wd(j).wait()
            def one(r, _):
                for c in load_gu(j, r):
                    c.wait()
                d = lax.dot_general(dh_v[part(r), :], wd_v[...], NT, preferred_element_type=f32).astype(bf).astype(f32)
                g, u = gu_v[r, 0], gu_v[r, 1]
                s = jax.nn.sigmoid(g)
                gs = g * s
                dg_v[part(r), :cg] = (d * u * (s + gs * (1.0 - s))).astype(bf)
                dg_v[part(r), cg:] = (d * gs).astype(bf)
                @pl.when(j + 1 < k.ng)
                def _():
                    for c in load_gu(j + 1, r): c.start()
                return 0
            lax.fori_loop(0, 2, one, 0)
            @pl.when(j + 1 < k.ng)
            def _():
                load_wd(j + 1).start()
            k.put_g(j, lax.dot_general(a_v[...], dg_v[...], TN, preferred_element_type=f32))
            k.sg.send(j)
        k.run(make_d, make_g)
    V, A, D, VM = pl.BlockSpec(memory_space=pltpu.VMEM), pl.BlockSpec(memory_space=pl.ANY), pltpu.SemaphoreType.DMA, pltpu.VMEM
    return pl.pallas_call(
        kernel, name="backward_first", out_shape=k.outs(), in_specs=[A] * 6, out_specs=[V] * 4,
        scratch_shapes=[VM((T, Dm), bf), VM((T, F), bf), VM((2, 2, rows, cg), f32), VM((T, 2 * cg), bf), VM((T, Dm), bf), VM((cg, Dm), bf),
                        D((4,)), D((2, 2)), D, *k.bufs()],
        compiler_params=pltpu.CompilerParams(collective_id=cid, has_side_effects=True, vmem_limit_bytes=67043328),
    )(a, act, gate, up, dh, wd)


def total(n, part, cid=9):
    def kernel(x_ref, o_ref, got, send, recv):
        me = lax.axis_index("dp")
        sem = pltpu.get_barrier_semaphore()
        def other(k):
            return lax.rem(me + k, n)
        def greet(k, _):
            pl.semaphore_signal(sem, inc=1, device_id={"dp": other(k)}, device_id_type=MESH)
            return 0
        lax.fori_loop(1, n, greet, 0)
        pl.semaphore_wait(sem, n - 1)
        def copy(k, slot):
            return pltpu.make_async_remote_copy(src_ref=x_ref, dst_ref=got.at[slot], send_sem=send.at[k], recv_sem=recv.at[slot], device_id={"dp": other(k)}, device_id_type=MESH)
        def start(k, _):
            copy(k, me).start()
            return 0
        lax.fori_loop(1, n, start, 0)
        got[me] = x_ref[...]
        def wait(k, _):
            copy(k, me).wait_send()
            copy(k, other(k)).wait_recv()
            return 0
        lax.fori_loop(1, n, wait, 0)
        o_ref[...] = jnp.sum(got[...], axis=0)
    V = pl.BlockSpec(memory_space=pltpu.VMEM)
    D = pltpu.SemaphoreType.DMA
    return pl.pallas_call(
        kernel, name="total", out_shape=jax.ShapeDtypeStruct(part.shape, jnp.float32), in_specs=[V], out_specs=V,
        scratch_shapes=[pltpu.VMEM((n, *part.shape), jnp.float32), D((n,)), D((n,))],
        compiler_params=pltpu.CompilerParams(collective_id=cid, has_side_effects=True),
    )(part)


def adamw(w, m, v, g):
    m = 0.9 * m + 0.1 * g
    v = 0.95 * v + 0.05 * g * g
    step = m * lax.rsqrt(v + 1e-8) + 0.1 * w
    return (w - 0.02 * step).astype(bf), m, v


def solution(mesh):
    n = mesh.shape["dp"]

    def step(x, dy, *arrays):
        weights, m, v = (arrays[i : i + 3] for i in (0, 3, 6))
        x, dy = x[0], dy[0]
        wgu, wd, g0, u0, act0, h1, a0, a1, act1, dg1, du1 = forward(n, x, dy, *weights, lag=2)
        *mine1, sq1, dh1 = backward_last(n, a1, act1, dg1, du1, dy, h1, wgu, 1)
        *mine0, sq0 = backward_first(n, a0, act0, g0, u0, dh1, wd, 0)
        squares = jnp.sum(total(n, sq0 + sq1))
        count = n * sum(w.size for w in weights)
        factor = jnp.minimum(1.0, 0.5 * lax.rsqrt(squares / count + 1e-30))
        gradients = [jnp.stack(g).astype(f32) * factor for g in zip(mine0, mine1, strict=True)]
        new = [adamw(w.astype(f32), m, v, g) for w, m, v, g in zip(weights, m, v, gradients, strict=True)]
        return tuple(one[which] for which in range(3) for one in new)

    states, cut = P(("rep", "dp"), None, None), P(None, "dp", None)
    return jax.shard_map(
        step,
        mesh=mesh,
        in_specs=(states, states) + (cut,) * 9,
        out_specs=(P("rep", "dp", None),) * 9,
        check_vma=False,
    )
```

```python
import functools, math
import jax, jax.numpy as jnp
from jax import lax
from jax.experimental import pallas as pl
from jax.experimental.pallas import tpu as pltpu
from jax.sharding import PartitionSpec as P
MESH = pl.DeviceIdType.MESH
bf = jnp.bfloat16

class Place:
    def __init__(self, n):
        self.side = side = math.isqrt(n // 2)
        me = lax.axis_index("dp")
        self.c = c = lax.rem(me, 2)
        chip = me // 2
        x, y = chip // side, lax.rem(chip, side)
        self.i1 = x + c * (y - x)
        self.i2 = y + c * (x - y)
        self.m1 = side + c * (1 - side)
        self.m2 = 1 + c * (side - 1)
        self.partner = me + 1 - 2 * c
    def mod(self, a):
        return lax.rem(a + 2 * self.side, self.side)
    def chip(self, j1, j2):
        return j1 * self.m1 + j2 * self.m2
    def next1(self, d):
        return 2 * self.chip(self.mod(self.i1 + d), self.i2) + self.c
    def next2(self, d):
        return 2 * self.chip(self.i1, self.mod(self.i2 + d)) + self.c

def barrier(p):
    sem = pltpu.get_barrier_semaphore()
    others = [p.partner, p.next1(1), p.next1(-1), p.next2(1), p.next2(-1)]
    for o in others:
        pl.semaphore_signal(sem, inc=1, device_id={"dp": o}, device_id_type=MESH)
    pl.semaphore_wait(sem, len(others))

DIRS = (1, -1)
BOTH = (0, 1)

class Gather:
    STAGES = 6

    def __init__(self, p, own, block, row, core, sent, local, sems):
        self.p, self.own, self.block, self.row, self.core, self.sent, self.local = p, own, block, row, core, sent, local
        self.sl, self.s, self.sd, self.r, self.rd = sems

    def remote(self, src, dst, s, r, dev):
        return pltpu.make_async_remote_copy(src_ref=src, dst_ref=dst, send_sem=s, recv_sem=r, device_id={"dp": dev}, device_id_type=MESH)

    def copy(self, k, j, e, core=0):
        p, d = self.p, DIRS[e]
        if k < 2:
            here = self.block(j, e, p.mod(p.i1 - d), p.i2) if k else self.block(j, None, p.i1, p.i2)
            src, to = here if k else self.own(j), p.next1(d)
        else:
            src = here = self.row(j, e, core, p.mod(p.i2 - d)) if k == 3 else self.row(j, None, core, p.i2)
            to = p.next2(d)
        return self.remote(src, here, self.s.at[k, e], self.r.at[j, k, e], to)

    def across(self, j, core):
        g = self.core(j, core)
        return self.remote(g, g, self.sd, self.rd.at[j], self.p.partner)

    def copies(self):
        return [pltpu.make_async_copy(a, b, self.sl.at[k]) for k, (a, b) in enumerate(self.local)]

    def begin(self):
        for c in self.copies():
            c.start()

    def stage(self, k, j):
        if k == self.STAGES - 1:
            self.across(j, 1 - self.p.c).wait_recv()
            return
        if k:
            for e in BOTH:
                self.copy(k - 1, j, e).wait_recv()
        if k < 2:
            for e in BOTH:
                self.copy(k, j, e).start()
        elif k < 4:
            if k == 2:
                @pl.when(j == 0)
                def _():
                    for c in self.copies():
                        c.wait()
            for core in BOTH:
                @pl.when(self.p.c == core)
                def _():
                    for e in BOTH:
                        self.copy(k, j, e, core).start()
        else:
            self.across(j, self.p.c).start()

    def end(self):
        *kinds, across = self.sent
        for k, view in enumerate(kinds):
            for e in BOTH:
                pltpu.make_async_copy(view, view, self.s.at[k, e]).wait()
        pltpu.make_async_copy(across, across, self.sd).wait()


def gather_sems(m, local):
    D = pltpu.SemaphoreType.DMA
    return [D((local,)), D((4, 2)), D, D((m, 4, 2)), D((m,))]


f32 = jnp.float32
TN = (((0,), (0,)), ((), ()))
NT = (((1,), (1,)), ((), ()))


class Scatter:
    STAGES = 6

    def __init__(self, p, lag, bufs, done):
        self.p, self.done = p, done
        self.own, self.q, self.mid, *self.bufs, self.sd, self.rd, self.s, self.r = bufs
        self.keep, self.pool = scatter_slots(self.q.shape[0], lag)

    def remote(self, src, dst, s, r, dev):
        return pltpu.make_async_remote_copy(src_ref=src, dst_ref=dst, send_sem=s, recv_sem=r, device_id={"dp": dev}, device_id_type=MESH)

    def slot(self, j, h):
        mine, other = lax.rem(j, self.keep), self.keep + lax.rem(j, self.pool)
        return mine + (other - mine) * (self.p.c + h - 2 * self.p.c * h)

    def across(self, j):
        return self.remote(self.own.at[self.keep + lax.rem(j, self.pool)], self.q.at[j], self.sd.at[j], self.rd.at[j], self.p.partner)

    def out(self, k):
        return self.bufs[2 * k]

    def got(self, k):
        return self.bufs[2 * k + 1]

    def at(self, j, ref):
        return lax.rem(j, ref.shape[0])

    def copy(self, k, j, e):
        to = self.p.next1(DIRS[e]) if k < 2 else self.p.next2(DIRS[e])
        return self.remote(self.out(k).at[self.at(j, self.out(k)), e], self.got(k).at[j, e], self.s.at[j, k, e], self.r.at[j, k, e], to)

    def send(self, j):
        self.across(j).start()

    def mine(self, j, e, j1, b):
        at = self.p.chip(j1, b)
        return self.own[lax.rem(j, self.keep), e, at].astype(f32) + self.q[j, e, at].astype(f32)

    def stage(self, k, j):
        p, n = self.p, self.p.side
        for c in [self.across(j)] if k == 1 else [self.copy(k - 2, j, e) for e in BOTH]:
            c.wait_recv()
            c.wait_send()
        m = self.at(j, self.mid)
        if k < 5:
            o, out = self.out(k - 1), self.at(j, self.out(k - 1))
        if k == 1:
            for e in BOTH:
                for b in range(n):
                    o[out, e, 0, b] = self.mine(j, e, p.mod(p.i1 + 2), b).astype(bf)
                    o[out, e, 1, b] = self.mine(j, 1 - e, p.mod(p.i1 + DIRS[e]), b).astype(bf)
        elif k == 2:
            for e in BOTH:
                for b in range(n):
                    o[out, e, b] = (self.got(0)[j, e, 0, b].astype(f32) + self.mine(j, e, p.mod(p.i1 + DIRS[e]), b)).astype(bf)
        elif k == 3:
            for h in BOTH:
                for b in range(n):
                    self.mid[m, h, b] = self.got(1)[j, h, b].astype(f32) + self.got(0)[j, 1 - h, 1, b].astype(f32) + self.mine(j, h, p.i1, b)
            for e in BOTH:
                o[out, e, 0] = self.mid[m, e, p.mod(p.i2 + 2)].astype(bf)
                o[out, e, 1] = self.mid[m, 1 - e, p.mod(p.i2 + DIRS[e])].astype(bf)
        elif k == 4:
            for e in BOTH:
                o[out, e] = (self.got(2)[j, e, 0].astype(f32) + self.mid[m, e, p.mod(p.i2 + DIRS[e])]).astype(bf)
        else:
            for h in BOTH:
                self.done(j, h, self.got(3)[j, h].astype(f32) + self.got(2)[j, 1 - h, 1].astype(f32) + self.mid[m, h, p.i2])
        if k < 5:
            for e in BOTH:
                self.copy(k - 1, j, e).start()


def scatter_slots(m, lag):
    return min(m, 3 * lag), min(m, lag)


def scatter_bufs(m, lag, side, R, C):
    keep, pool = scatter_slots(m, lag)
    few, V, D = min(m, lag), pltpu.VMEM, pltpu.SemaphoreType.DMA
    pairs = [V((k, 2, *s, R, C), bf) for s in ((2, side), (side,), (2,), ()) for k in (few, m)]
    return [V((keep + pool, 2, side * side, R, C), bf), V((m, 2, side * side, R, C), bf), V((min(m, 2 * lag), 2, side, R, C), f32), *pairs,
            D((m,)), D((m,)), D((m, 4, 2)), D((m, 4, 2))]


def normed_rows(h):
    wide = h.astype(f32)
    scale = lax.rsqrt(jnp.mean(wide * wide, -1, keepdims=True) + 1e-6)
    return (wide * scale).astype(bf)


def forward(n, x, dy, wg, wu, wd, lag=2, cg=256, cd=128, cid=1):
    side = math.isqrt(n // 2)
    T, Dm = x.shape
    L, R, F = wg.shape
    Rd = wd.shape[1]
    ng, nd, rows, tile = F // cg, Dm // (2 * cd), T // 2, T // 8
    width = 2 * cd

    def kernel(x_h, dy_h, wg_ref, wu_ref, wd_ref, ogu, od, g0, u0, act0, h1, a0, a1, act1, dgu1,
               xv, av, dyv, actv, own_v, wb, wdb, wdr, stg, st3, s_in, s_w, s_wd, s_wr, s_stg, s_act, s_out, s_st3, *sems):
        p = Place(n)
        pltpu.make_async_copy(x_h, xv, s_in.at[0]).start()
        pltpu.make_async_copy(dy_h, dyv, s_in.at[1]).start()
        own_v[:, 0] = wg_ref[...]
        own_v[:, 1] = wu_ref[...]
        barrier(p)
        every = slice(None)

        def cols(j, w):
            return pl.ds(pl.multiple_of(j * w, w), w)
        def core_rows(c):
            return pl.ds(c * Rd if isinstance(c, int) else pl.multiple_of(c * Rd, 8), Rd)
        def place(q, m):
            return q // m, lax.rem(q, m)

        def at_g(q, e, x, y, c):
            l, j = place(q, ng)
            return ogu.at[l, x, y, c, every if e is None else e, every, cols(j, cg)]
        def at_d(q, e, x, y, c):
            l, j = place(q, nd)
            return od.at[l, x, y, core_rows(c), cols(j, width) if e is None else cols(2 * j + e, cd)]
        def own_g(q):
            l, j = place(q, ng)
            return own_v.at[l, every, every, cols(j, cg)]
        def own_d(q):
            l, j = place(q, nd)
            return wd_ref.at[l, every, cols(j, width)]

        def stream(at, own, sent, local, sems):
            x, y = p.i1 + p.c * (p.i2 - p.i1), p.i2 + p.c * (p.i1 - p.i2)
            def block(q, e, j1, j2):
                return at(q, e, j1 + p.c * (j2 - j1), j2 + p.c * (j1 - j2), p.c)
            def row(q, e, core, j2):
                return at(q, e, j2, every, core) if core else at(q, e, every, j2, core)
            def core(q, c):
                return at(q, None, every, every, c)
            return Gather(p, own, block, row, core, sent, local(x, y), sems)

        r0, h0 = core_rows(0), pl.ds(0, Dm // 2)
        sent_g = [ogu.at[:, 0, 0, 0], ogu.at[:, 0, 0, 0, 0], ogu.at[:, :, 0, 0], ogu.at[:, :, 0, 0, 0], ogu.at[:, :, :, 0]]
        sent_d = [od.at[:, 0, 0, r0], od.at[:, 0, 0, r0, h0], od.at[:, :, 0, r0], od.at[:, :, 0, r0, h0], od.at[:, :, :, r0]]
        G = stream(at_g, own_g, sent_g, lambda x, y: [(own_v.at[l], ogu.at[l, x, y, p.c]) for l in range(L)], sems[:5])
        Ds = stream(at_d, own_d, sent_d, lambda x, y: [(wd_ref.at[l], od.at[l, x, y, core_rows(p.c)]) for l in range(L)], sems[5:])
        G.begin()
        Ds.begin()
        downs = 2 * nd
        chunks, depth = 2 * ng + downs, (Gather.STAGES - 1) * lag

        def load_g(q):
            l, j = place(q, ng)
            return pltpu.make_async_copy(ogu.at[l, :, :, :, :, :, cols(j, cg)], wb.at[lax.rem(q, 2)], s_w.at[lax.rem(q, 2)])
        def load_d(j):
            return pltpu.make_async_copy(od.at[0, :, :, :, cols(j, width)], wdb.at[lax.rem(j, 2)], s_wd.at[lax.rem(j, 2)])
        def load_r(k):
            return pltpu.make_async_copy(od.at[1, k // side, lax.rem(k, side)], wdr.at[pl.ds(pl.multiple_of(k * 2 * Rd, 2 * Rd), 2 * Rd)], s_wr.at[k])
        def weights(q, e):
            return wb[lax.rem(q, 2), :, :, :, e].reshape(Dm, cg)
        def part(r):
            return pl.ds(pl.multiple_of(r * rows, rows), rows)
        def put_g(j, r):
            return [pltpu.make_async_copy(stg.at[r, e], (g0, u0)[e].at[part(r), cols(j, cg)], s_stg.at[r, e]) for e in BOTH]
        def put_act(j):
            return pltpu.make_async_copy(actv.at[:, cols(j, cg)], act0.at[:, cols(j, cg)], s_act.at[j])
        def put_3(j, r):
            to = [act1.at[part(r), cols(j, cg)], *(dgu1.at[e, part(r), cols(j, cg)] for e in BOTH)]
            return [pltpu.make_async_copy(st3.at[r, e], ref, s_st3.at[r, e]) for e, ref in enumerate(to)]
        put_a0 = pltpu.make_async_copy(av, a0, s_out.at[0])
        put_h1 = pltpu.make_async_copy(xv, h1, s_out.at[1])
        put_a1 = pltpu.make_async_copy(av, a1, s_out.at[2])

        def norm():
            def one(r, _):
                rs_ = pl.ds(pl.multiple_of(r * tile, tile), tile)
                av[rs_, :] = normed_rows(xv[rs_, :])
                return 0
            lax.fori_loop(0, T // tile, one, 0)

        def first():
            pltpu.make_async_copy(x_h, xv, s_in.at[0]).wait()
            pltpu.make_async_copy(dy_h, dyv, s_in.at[1]).wait()
            norm()
            put_a0.start()

        def gate_up(j):
            load_g(j).wait()
            def one(r, _):
                @pl.when(j > 0)
                def _():
                    for c in put_g(j - 1, r):
                        c.wait()
                a = av[part(r), :]
                g = jnp.dot(a, weights(j, 0), preferred_element_type=f32)
                u = jnp.dot(a, weights(j, 1), preferred_element_type=f32)
                s = jax.nn.sigmoid(g)
                gs = g * s
                stg[r, 0] = u * (s + gs * (1.0 - s))
                stg[r, 1] = gs
                actv[part(r), cols(j, cg)] = (gs * u).astype(bf)
                for c in put_g(j, r):
                    c.start()
                return 0
            lax.fori_loop(0, 2, one, 0)
            put_act(j).start()

        def down(j):
            load_d(j).wait()
            def one(r, _):
                y = jnp.dot(actv[part(r), :], wdb[lax.rem(j, 2)].reshape(F, width), preferred_element_type=f32).astype(bf)
                xv[part(r), cols(j, width)] = xv[part(r), cols(j, width)] + y
                return 0
            lax.fori_loop(0, 2, one, 0)

        def second():
            for r in BOTH:
                for c in put_g(ng - 1, r):
                    c.wait()
            put_a0.wait()
            put_h1.start()
            norm()
            put_a1.start()

        def gate_up_back(j):
            load_g(ng + j).wait()
            @pl.when(j == 0)
            def _():
                def wait(k, _):
                    load_r(k).wait()
                    return 0
                lax.fori_loop(0, side * side, wait, 0)
            def one(r, _):
                @pl.when(j > 0)
                def _():
                    for c in put_3(j - 1, r):
                        c.wait()
                a = av[part(r), :]
                g = jnp.dot(a, weights(ng + j, 0), preferred_element_type=f32)
                u = jnp.dot(a, weights(ng + j, 1), preferred_element_type=f32)
                d = lax.dot_general(dyv[part(r), :], wdr[cols(j, cg), :], NT, preferred_element_type=f32).astype(bf).astype(f32)
                s = jax.nn.sigmoid(g)
                gs = g * s
                st3[r, 0] = (gs * u).astype(bf)
                st3[r, 1] = (d * u * (s + gs * (1.0 - s))).astype(bf)
                st3[r, 2] = (d * gs).astype(bf)
                for c in put_3(j, r):
                    c.start()
                return 0
            lax.fori_loop(0, 2, one, 0)

        def tick(t, _):
            for k in reversed(range(Gather.STAGES)):
                q = t - k * lag
                late = q >= ng + downs
                @pl.when((q >= 0) & (q < chunks) & ((q < ng) | late))
                def _():
                    j = q - jnp.where(late, downs, 0)
                    G.stage(k, j)
                    if k == Gather.STAGES - 1:
                        load_g(j).start()
                @pl.when((q >= ng) & (q < ng + downs))
                def _():
                    j = q - ng
                    Ds.stage(k, j)
                    if k == Gather.STAGES - 1:
                        @pl.when(j < nd)
                        def _():
                            load_d(j).start()
                        @pl.when(j == downs - 1)
                        def _():
                            def start(k, _):
                                load_r(k).start()
                                return 0
                            lax.fori_loop(0, side * side, start, 0)
            @pl.when(t == min(2, lag - 1))
            def _():
                first()
            m = t - depth - 1
            @pl.when((m >= 0) & (m < ng))
            def _():
                gate_up(m)
            @pl.when((m >= ng) & (m < ng + nd))
            def _():
                down(m - ng)
            @pl.when(m == ng + nd)
            def _():
                second()
            @pl.when(m >= ng + downs)
            def _():
                gate_up_back(m - ng - downs)
            return 0
        lax.fori_loop(0, chunks + depth + 1, tick, 0)
        for r in BOTH:
            for c in put_3(ng - 1, r):
                c.wait()
        G.end()
        Ds.end()
        def last(j, _):
            put_act(j).wait()
            return 0
        lax.fori_loop(0, ng, last, 0)
        put_h1.wait()
        put_a1.wait()

    S, V, A, D = jax.ShapeDtypeStruct, pl.BlockSpec(memory_space=pltpu.VMEM), pl.BlockSpec(memory_space=pl.ANY), pltpu.SemaphoreType.DMA
    VM = pltpu.VMEM
    sems = gather_sems(L * ng, L) + gather_sems(L * nd, L)
    wide, thin = S((T, F), bf), S((T, Dm), bf)
    out = pl.pallas_call(
        kernel, name="forward",
        out_shape=[S((L, side, side, 2, 2, R, F), bf), S((L, side, side, 2 * Rd, Dm), bf),
                   S((T, F), f32), S((T, F), f32), wide, thin, thin, thin, wide, S((2, T, F), bf)],
        in_specs=[A, A, V, V, V], out_specs=[A] * 10,
        scratch_shapes=[VM((T, Dm), bf), VM((T, Dm), bf), VM((T, Dm), bf), VM((T, F), bf), VM((L, 2, R, F), bf), VM((2, side, side, 2, 2, R, cg), bf), VM((2, side, side, 2 * Rd, width), bf), VM((F, Dm), bf),
                        VM((2, 2, rows, cg), f32), VM((2, 3, rows, cg), bf),
                        D((2,)), D((2,)), D((2,)), D((side * side,)), D((2, 2)), D((ng,)), D((3,)), D((2, 3)), *sems],
        compiler_params=pltpu.CompilerParams(collective_id=cid, has_side_effects=True, vmem_limit_bytes=67043328),
    )(x, dy, wg, wu, wd)
    ogu, od, *rest = out
    return ogu, od.reshape(L, n * Rd, Dm), *rest


def greet_all(n):
    me, sem = lax.axis_index("dp"), pltpu.get_barrier_semaphore()
    def greet(k, _):
        pl.semaphore_signal(sem, inc=1, device_id={"dp": lax.rem(me + k, n)}, device_id_type=MESH)
        return 0
    lax.fori_loop(1, n, greet, 0)
    pl.semaphore_wait(sem, n - 1)


def clip(n, count, part, o_ref, x_ref, got, send, recv):
    me = lax.axis_index("dp")
    x_ref[...] = part
    def copy(k, slot):
        return pltpu.make_async_remote_copy(src_ref=x_ref, dst_ref=got.at[slot], send_sem=send.at[k], recv_sem=recv.at[slot], device_id={"dp": lax.rem(me + k, n)}, device_id_type=MESH)
    def start(k, _):
        copy(k, me).start()
        return 0
    lax.fori_loop(1, n, start, 0)
    got[me] = part
    def wait(k, _):
        copy(k, me).wait_send()
        copy(k, lax.rem(me + k, n)).wait_recv()
        return 0
    lax.fori_loop(1, n, wait, 0)
    o_ref[...] = jnp.minimum(1.0, 0.5 * lax.rsqrt(jnp.full_like(part, jnp.sum(got[...])) / count + 1e-30))


def update(factor, weights, moments, squares, grads):
    L = len(grads)
    def kernel(f_ref, *refs):
        f, layer = f_ref[0, 0], pl.program_id(0)
        ins, outs = refs[:-9], refs[-9:]
        for i in range(3):
            w, m, v = (ins[3 * k + i][0].astype(jnp.float32) for k in range(3))
            g = ins[9 + i][...].astype(jnp.float32)
            for l in range(1, L):
                g = jnp.where(layer == l, ins[9 + 3 * l + i][...].astype(jnp.float32), g)
            g = g * f
            m = 0.9 * m + 0.1 * g
            v = 0.95 * v + 0.05 * g * g
            step = m * lax.rsqrt(v + 1e-8) + 0.1 * w
            outs[i][0] = (w - 0.02 * step).astype(bf)
            outs[3 + i][0] = m
            outs[6 + i][0] = v
    def whole(a):
        return pl.BlockSpec((1, a.shape[1], a.shape[2] // 2), lambda l, c: (l, 0, c))
    arrays = (*weights, *moments, *squares)
    flat = [g for layer in grads for g in layer]
    S = jax.ShapeDtypeStruct
    return pl.pallas_call(
        kernel, name="update", grid=(L, 2),
        out_shape=[S(a.shape, a.dtype) for a in arrays],
        in_specs=[pl.BlockSpec(memory_space=pltpu.SMEM), *map(whole, arrays), *(pl.BlockSpec((g.shape[0], g.shape[1] // 2), lambda l, c: (0, c)) for g in flat)],
        out_specs=[*map(whole, arrays)],
    )(factor, *arrays, *flat)


class Layer:
    def __init__(self, n, a, act, lag, lagd, cg, cd):
        self.n, self.side = n, math.isqrt(n // 2)
        self.T, self.Dm = a.shape
        self.F = act.shape[1]
        self.R, self.Rd, self.ng, self.nd = self.Dm // n, self.F // n, self.F // cg, self.Dm // (2 * cd)
        self.lag, self.lagd, self.cg, self.cd, self.half, self.chips = lag, lagd, cg, cd, self.F // 2, self.side * self.side
    def bufs(self):
        return [*scatter_bufs(self.nd, self.lagd, self.side, self.Rd, self.cd), *scatter_bufs(self.ng, self.lag, self.side, self.R, self.cg)]
    def outs(self):
        S = jax.ShapeDtypeStruct
        return [S((self.R, self.F), bf), S((self.R, self.F), bf), S((self.Rd, self.Dm), bf), S((8, 128), f32)]
    def streams(self, p, og, ou, od, sq, bufs):
        def add(v):
            w = v.astype(f32)
            w = jnp.sum((w * w).reshape(w.shape[0] // 8, 8, w.shape[1]), 0)
            for k in range(w.shape[1] // 128):
                sq[...] += w[:, 128 * k:128 * k + 128]
        def done_d(j, e, v):
            v = v.astype(bf)
            od[:, pl.ds(pl.multiple_of((2 * j + e) * self.cd, self.cd), self.cd)] = v
            add(v)
        def done_g(j, e, v):
            v = v.astype(bf)
            (og, ou)[e][:, pl.ds(pl.multiple_of(j * self.cg, self.cg), self.cg)] = v
            add(v)
        sq[...] = jnp.zeros_like(sq)
        self.p = p
        split = len(bufs) // 2
        self.sd = Scatter(p, self.lagd, bufs[:split], done_d)
        self.sg = Scatter(p, self.lag, bufs[split:], done_g)
    def put_d(self, j, m, val):
        for e in BOTH:
            v = val[:, e * self.cd:(e + 1) * self.cd].reshape(self.chips // 2, 2, self.Rd, self.cd).astype(bf)
            for h in BOTH:
                self.sd.own[self.sd.slot(j, h), e, m * self.chips // 2:(m + 1) * self.chips // 2] = v[:, h]
    def put_g(self, j, val):
        for e in BOTH:
            v = val[:, e * self.cg:(e + 1) * self.cg].reshape(self.chips, 2, self.R, self.cg).astype(bf)
            for h in BOTH:
                self.sg.own[self.sg.slot(j, h), e] = v[:, h]
    def run(self, make_d, make_g, extra=0, more=None):
        streams = ((self.sd, self.nd, 0, self.lagd, make_d), (self.sg, self.ng, self.nd, self.lag, make_g))
        total = max(lo + m + (Scatter.STAGES - 1) * lg for _, m, lo, lg, _ in streams)
        total = max(total, self.nd + self.ng + extra)
        def body(i, _):
            for k in reversed(range(Scatter.STAGES)):
                for s, m, lo, lg, make in streams:
                    j = i - lo - k * lg
                    @pl.when((j >= 0) & (j < m))
                    def _():
                        make(j) if k == 0 else s.stage(k, j)
            if extra:
                j = i - self.nd - self.ng
                @pl.when((j >= 0) & (j < extra))
                def _():
                    more(j)
            return 0
        lax.fori_loop(0, total, body, 0)


def tall_product(ref, lo, hi, rhs, most=768):
    return jnp.concatenate([lax.dot_general(ref[:rhs.shape[0], m:min(m + most, hi)], rhs, TN, preferred_element_type=f32) for m in range(lo, hi, most)], 0)


def cols_of(j, w):
    return pl.ds(pl.multiple_of(j * w, w), w)


def backward_last(n, a, act, dgu, dy, h, wgu, layer, lag=2, lagd=2, cg=256, cd=128, cid=2):
    k = Layer(n, a, act, lag, lagd, cg, cd)
    T, Dm, F, tile = k.T, k.Dm, k.F, k.T // k.nd
    def kernel(a_h, act_h, dgu_h, dy_h, h_h, w_h, og, ou, od, sq, dh_h,
               a_v, act_v, dg_v, dy_v, row_v, part_v, ld, ldg, ldy, ldr, ldo, ldw, *bufs):
        p = Place(n)
        def load_act(m):
            cols = pl.ds(m * k.half, k.half)
            return pltpu.make_async_copy(act_h.at[:, cols], act_v.at[:T, cols], ld.at[m])
        load_a = pltpu.make_async_copy(a_h, a_v, ld.at[2])
        def load_dy(j):
            return pltpu.make_async_copy(dy_h.at[:, cols_of(j, 2 * cd)], dy_v.at[lax.rem(j, 2)], ldy.at[lax.rem(j, 2)])
        def load_dg(j, e):
            return pltpu.make_async_copy(dgu_h.at[e, :, cols_of(j, cg)], dg_v.at[lax.rem(j, 2), :, e * cg:(e + 1) * cg], ldg.at[lax.rem(j, 2), e])
        def load_w(d):
            for e in BOTH:
                chip = d // 2
                rows = pl.ds(pl.multiple_of((e * n + d) * k.R, k.R), k.R)
                pltpu.make_async_copy(w_h.at[layer, chip // k.side, lax.rem(chip, k.side), lax.rem(d, 2), e], act_v.at[rows], ldw).start()
            return 0
        w_v = act_v.at[:2 * Dm]
        def load_row(r, e):
            return pltpu.make_async_copy(dgu_h.at[e, cols_of(r, tile), :], row_v.at[e], ldr.at[e])
        def blocks(ref, r, v):
            return [(ref.at[cols_of(r, tile), c * 2 * cd:(c + 1) * 2 * cd], v.at[c * tile:(c + 1) * tile]) for c in range(k.nd)]
        h_v, y_v = dy_v.at[0], dy_v.at[1]
        def load_tile(ref, r, v, sem):
            for src, dst in blocks(ref, r, v):
                pltpu.make_async_copy(src, dst, sem).start()
        def load_h(r):
            load_tile(h_h, r, h_v, ldr.at[2])
        def load_y(r):
            load_tile(dy_h, r, y_v, ldr.at[3])
        def put(r):
            for dst, src in blocks(dh_h, r, y_v):
                pltpu.make_async_copy(src, dst, ldo).start()
        def arrived(v, sem):
            pltpu.make_async_copy(v, v, sem).wait()
        def tile_of(v, m):
            return jnp.concatenate([v[pl.ds(pl.multiple_of(c * tile + m * part, part), part)] for c in range(k.nd)], 1)
        part = tile // 4
        load_dy(0).start(); load_act(0).start(); load_act(1).start()
        barrier(p)
        k.streams(p, og, ou, od, sq, bufs)
        load_dy(0).wait(); load_act(0).wait()
        def make_d(j):
            @pl.when(j + 1 < k.nd)
            def _(): load_dy(j + 1).start()
            @pl.when(j == 0)
            def _(): load_a.start()
            @pl.when(j == k.nd - 1)
            def _():
                for e in BOTH: load_dg(0, e).start()
            for m in BOTH:
                if m == 1:
                    @pl.when(j == 0)
                    def _(): load_act(1).wait()
                k.put_d(j, m, tall_product(act_v, m * k.half, (m + 1) * k.half, dy_v[lax.rem(j, 2)]))
            k.sd.send(j)
            @pl.when(j + 1 < k.nd)
            def _(): load_dy(j + 1).wait()
        def make_g(j):
            @pl.when(j + 1 < k.ng)
            def _():
                for e in BOTH: load_dg(j + 1, e).start()
            @pl.when(j == 0)
            def _():
                lax.fori_loop(0, n, lambda d, _: load_w(d), 0)
                load_a.wait()
            @pl.when(j == k.ng - 1)
            def _():
                for e in BOTH: load_row(0, e).start()
                load_h(0)
                load_y(0)
            for e in BOTH:
                load_dg(j, e).wait()
            k.put_g(j, lax.dot_general(a_v[...], dg_v[lax.rem(j, 2)], TN, preferred_element_type=f32))
            k.sg.send(j)
        def rows(i):
            r, e = i // 2, lax.rem(i, 2)
            @pl.when(i == 0)
            def _():
                pltpu.make_async_copy(w_v, w_v, ldw).wait()
            @pl.when((e == 0) & (r > 0))
            def _():
                arrived(y_v, ldo)
                load_y(r)
            load_row(r, e).wait()
            part_v[e] = lax.dot_general(row_v[e], act_v[pl.ds(pl.multiple_of(e * Dm, Dm), Dm)], NT, preferred_element_type=f32).astype(bf)
            @pl.when(r + 1 < T // tile)
            def _():
                load_row(r + 1, e).start()
            @pl.when(e == 1)
            def _():
                arrived(h_v, ldr.at[2])
                arrived(y_v, ldr.at[3])
                def one(m, _):
                    some = cols_of(m, part)
                    da = (part_v[0, some] + part_v[1, some]).astype(f32)
                    wide = tile_of(h_v, m).astype(f32)
                    s = lax.rsqrt(jnp.mean(wide * wide, -1, keepdims=True) + 1e-6)
                    t = jnp.sum(da * wide, -1, keepdims=True) * (s * s * s) * (1.0 / Dm)
                    new = (da * s - wide * t).astype(bf) + tile_of(y_v, m)
                    for c in range(k.nd):
                        y_v[pl.ds(pl.multiple_of(c * tile + m * part, part), part)] = new[:, c * 2 * cd:(c + 1) * 2 * cd]
                    return 0
                lax.fori_loop(0, 4, one, 0)
                put(r)
                @pl.when(r + 1 < T // tile)
                def _():
                    load_h(r + 1)
        k.run(make_d, make_g, 2 * (T // tile), rows)
        arrived(y_v, ldo)
    V, A, D, VM = pl.BlockSpec(memory_space=pltpu.VMEM), pl.BlockSpec(memory_space=pl.ANY), pltpu.SemaphoreType.DMA, pltpu.VMEM
    return pl.pallas_call(
        kernel, name="backward_last", out_shape=[*k.outs(), jax.ShapeDtypeStruct((T, Dm), bf)], in_specs=[A] * 6, out_specs=[V] * 4 + [A],
        scratch_shapes=[VM((T, Dm), bf), VM((max(T, 2 * Dm), F), bf), VM((2, T, 2 * cg), bf), VM((2, T, 2 * cd), bf), VM((2, tile, F), bf), VM((2, tile, Dm), bf),
                        D((3,)), D((2, 2)), D((2,)), D((4,)), D, D, *k.bufs()],
        compiler_params=pltpu.CompilerParams(collective_id=cid, has_side_effects=True, vmem_limit_bytes=67043328),
    )(a, act, dgu, dy, h, wgu)


def backward_first(n, a, act, by_gate, by_up, dh, wd, sq_last, count, layer, lag=2, lagd=2, cg=256, cd=128, cid=3):
    k = Layer(n, a, act, lag, lagd, cg, cd)
    T, Dm, F, rows = k.T, k.Dm, k.F, k.T // 2
    def kernel(a_h, act_h, g_h, u_h, dh_h, wd_h, sq_ref, og, ou, od, factor, a_v, act_v, gu_v, dg_v, dh_v, wd_v, ld, ldg, ldw, sq, part_v, got, send, recv, *bufs):
        p = Place(n)
        def load_act(m):
            cols = pl.ds(m * k.half, k.half)
            return pltpu.make_async_copy(act_h.at[:, cols], act_v.at[:, cols], ld.at[m])
        load_a = pltpu.make_async_copy(a_h, a_v, ld.at[2])
        load_dh = pltpu.make_async_copy(dh_h, dh_v, ld.at[3])
        def part(r):
            return pl.ds(pl.multiple_of(r * rows, rows), rows)
        def load_gu(j, r):
            return [pltpu.make_async_copy((g_h, u_h)[e].at[part(r), cols_of(j, cg)], gu_v.at[r, e], ldg.at[r, e]) for e in BOTH]
        def load_wd(j):
            return pltpu.make_async_copy(wd_h.at[layer, cols_of(j, cg), :], wd_v, ldw)
        load_dh.start(); load_act(0).start(); load_act(1).start()
        greet_all(n)
        k.streams(p, og, ou, od, sq, bufs)
        load_dh.wait(); load_act(0).wait()
        def make_d(j):
            @pl.when(j == 0)
            def _(): load_a.start()
            @pl.when(j == k.nd - 1)
            def _():
                for r in BOTH:
                    for c in load_gu(0, r): c.start()
                load_wd(0).start()
            for m in BOTH:
                if m == 1:
                    @pl.when(j == 0)
                    def _(): load_act(1).wait()
                k.put_d(j, m, tall_product(act_v, m * k.half, (m + 1) * k.half, dh_v[:, cols_of(j, 2 * cd)]))
            k.sd.send(j)
        def make_g(j):
            @pl.when(j == 0)
            def _(): load_a.wait()
            load_wd(j).wait()
            def one(r, _):
                for c in load_gu(j, r):
                    c.wait()
                d = lax.dot_general(dh_v[part(r), :], wd_v[...], NT, preferred_element_type=f32).astype(bf).astype(f32)
                for e in BOTH:
                    dg_v[part(r), e * cg:(e + 1) * cg] = (d * gu_v[r, e]).astype(bf)
                @pl.when(j + 1 < k.ng)
                def _():
                    for c in load_gu(j + 1, r): c.start()
                return 0
            lax.fori_loop(0, 2, one, 0)
            @pl.when(j + 1 < k.ng)
            def _():
                load_wd(j + 1).start()
            k.put_g(j, lax.dot_general(a_v[...], dg_v[...], TN, preferred_element_type=f32))
            k.sg.send(j)
        k.run(make_d, make_g)
        clip(n, count, sq[...] + sq_ref[...], factor, part_v, got, send, recv)
    V, A, D, VM = pl.BlockSpec(memory_space=pltpu.VMEM), pl.BlockSpec(memory_space=pl.ANY), pltpu.SemaphoreType.DMA, pltpu.VMEM
    return pl.pallas_call(
        kernel, name="backward_first", out_shape=k.outs(), in_specs=[A] * 6 + [V], out_specs=[V] * 4,
        scratch_shapes=[VM((T, Dm), bf), VM((T, F), bf), VM((2, 2, rows, cg), f32), VM((T, 2 * cg), bf), VM((T, Dm), bf), VM((cg, Dm), bf),
                        D((4,)), D((2, 2)), D, VM((8, 128), f32), VM((8, 128), f32), VM((n, 8, 128), f32), D((n,)), D((n,)), *k.bufs()],
        compiler_params=pltpu.CompilerParams(collective_id=cid, has_side_effects=True, vmem_limit_bytes=67043328),
    )(a, act, by_gate, by_up, dh, wd, sq_last)


def solution(mesh):
    n = mesh.shape["dp"]

    def step(x, dy, *arrays):
        weights, m, v = (arrays[i : i + 3] for i in (0, 3, 6))
        x, dy = x[0], dy[0]
        wgu, wd, g0, u0, act0, h1, a0, a1, act1, dgu1 = forward(n, x, dy, *weights)
        *mine1, sq1, dh1 = backward_last(n, a1, act1, dgu1, dy, h1, wgu, 1)
        *mine0, factor = backward_first(n, a0, act0, g0, u0, dh1, wd, sq1, n * sum(w.size for w in weights), 0)
        return tuple(update(factor, weights, m, v, (mine0, mine1)))

    states, cut = P(("rep", "dp"), None, None), P(None, "dp", None)
    return jax.shard_map(
        step,
        mesh=mesh,
        in_specs=(states, states) + (cut,) * 9,
        out_specs=(P("rep", "dp", None),) * 9,
        check_vma=False,
    )
```

```python
import functools, math
import jax, jax.numpy as jnp
from jax import lax
from jax.experimental import pallas as pl
from jax.experimental.pallas import tpu as pltpu
from jax.sharding import PartitionSpec as P
MESH = pl.DeviceIdType.MESH
bf = jnp.bfloat16

class Place:
    def __init__(self, n):
        self.side = side = math.isqrt(n // 2)
        me = lax.axis_index("dp")
        self.c = c = lax.rem(me, 2)
        chip = me // 2
        x, y = chip // side, lax.rem(chip, side)
        self.i1 = x + c * (y - x)
        self.i2 = y + c * (x - y)
        self.m1 = side + c * (1 - side)
        self.m2 = 1 + c * (side - 1)
        self.partner = me + 1 - 2 * c
    def mod(self, a):
        return lax.rem(a + 2 * self.side, self.side)
    def chip(self, j1, j2):
        return j1 * self.m1 + j2 * self.m2
    def next1(self, d):
        return 2 * self.chip(self.mod(self.i1 + d), self.i2) + self.c
    def next2(self, d):
        return 2 * self.chip(self.i1, self.mod(self.i2 + d)) + self.c

def barrier(p):
    sem = pltpu.get_barrier_semaphore()
    others = [p.partner, p.next1(1), p.next1(-1), p.next2(1), p.next2(-1)]
    for o in others:
        pl.semaphore_signal(sem, inc=1, device_id={"dp": o}, device_id_type=MESH)
    pl.semaphore_wait(sem, len(others))

DIRS = (1, -1)
BOTH = (0, 1)

class Gather:
    STAGES = 6

    def __init__(self, p, own, block, row, core, sent, local, sems):
        self.p, self.own, self.block, self.row, self.core, self.sent, self.local = p, own, block, row, core, sent, local
        self.sl, self.s, self.sd, self.r, self.rd = sems

    def remote(self, src, dst, s, r, dev):
        return pltpu.make_async_remote_copy(src_ref=src, dst_ref=dst, send_sem=s, recv_sem=r, device_id={"dp": dev}, device_id_type=MESH)

    def copy(self, k, j, e, core=0):
        p, d = self.p, DIRS[e]
        if k < 2:
            here = self.block(j, e, p.mod(p.i1 - d), p.i2) if k else self.block(j, None, p.i1, p.i2)
            src, to = here if k else self.own(j), p.next1(d)
        else:
            src = here = self.row(j, e, core, p.mod(p.i2 - d)) if k == 3 else self.row(j, None, core, p.i2)
            to = p.next2(d)
        return self.remote(src, here, self.s.at[k, e], self.r.at[j, k, e], to)

    def across(self, j, core):
        g = self.core(j, core)
        return self.remote(g, g, self.sd, self.rd.at[j], self.p.partner)

    def copies(self):
        return [pltpu.make_async_copy(a, b, self.sl.at[k]) for k, (a, b) in enumerate(self.local)]

    def begin(self):
        for c in self.copies():
            c.start()

    def stage(self, k, j):
        if k == self.STAGES - 1:
            self.across(j, 1 - self.p.c).wait_recv()
            return
        if k:
            for e in BOTH:
                self.copy(k - 1, j, e).wait_recv()
        if k < 2:
            for e in BOTH:
                self.copy(k, j, e).start()
        elif k < 4:
            if k == 2:
                @pl.when(j == 0)
                def _():
                    for c in self.copies():
                        c.wait()
            for core in BOTH:
                @pl.when(self.p.c == core)
                def _():
                    for e in BOTH:
                        self.copy(k, j, e, core).start()
        else:
            self.across(j, self.p.c).start()

    def end(self):
        *kinds, across = self.sent
        for k, view in enumerate(kinds):
            for e in BOTH:
                pltpu.make_async_copy(view, view, self.s.at[k, e]).wait()
        pltpu.make_async_copy(across, across, self.sd).wait()


def gather_sems(m, local):
    D = pltpu.SemaphoreType.DMA
    return [D((local,)), D((4, 2)), D, D((m, 4, 2)), D((m,))]


f32 = jnp.float32
TN = (((0,), (0,)), ((), ()))
NT = (((1,), (1,)), ((), ()))


class Scatter:
    STAGES = 6

    def __init__(self, p, lag, bufs, done):
        self.p, self.done = p, done
        self.own, self.q, self.mid, *self.bufs, self.sd, self.rd, self.s, self.r = bufs
        self.keep, self.pool = scatter_slots(self.q.shape[0], lag)

    def remote(self, src, dst, s, r, dev):
        return pltpu.make_async_remote_copy(src_ref=src, dst_ref=dst, send_sem=s, recv_sem=r, device_id={"dp": dev}, device_id_type=MESH)

    def slot(self, j, h):
        mine, other = lax.rem(j, self.keep), self.keep + lax.rem(j, self.pool)
        return mine + (other - mine) * (self.p.c + h - 2 * self.p.c * h)

    def across(self, j):
        return self.remote(self.own.at[self.keep + lax.rem(j, self.pool)], self.q.at[j], self.sd.at[j], self.rd.at[j], self.p.partner)

    def out(self, k):
        return self.bufs[2 * k]

    def got(self, k):
        return self.bufs[2 * k + 1]

    def at(self, j, ref):
        return lax.rem(j, ref.shape[0])

    def copy(self, k, j, e):
        to = self.p.next1(DIRS[e]) if k < 2 else self.p.next2(DIRS[e])
        return self.remote(self.out(k).at[self.at(j, self.out(k)), e], self.got(k).at[j, e], self.s.at[j, k, e], self.r.at[j, k, e], to)

    def send(self, j):
        self.across(j).start()

    def mine(self, j, e, j1, b):
        at = self.p.chip(j1, b)
        return self.own[lax.rem(j, self.keep), e, at].astype(f32) + self.q[j, e, at].astype(f32)

    def stage(self, k, j):
        p, n = self.p, self.p.side
        for c in [self.across(j)] if k == 1 else [self.copy(k - 2, j, e) for e in BOTH]:
            c.wait_recv()
            c.wait_send()
        m = self.at(j, self.mid)
        if k < 5:
            o, out = self.out(k - 1), self.at(j, self.out(k - 1))
        if k == 1:
            for e in BOTH:
                for b in range(n):
                    o[out, e, 0, b] = self.mine(j, e, p.mod(p.i1 + 2), b).astype(bf)
                    o[out, e, 1, b] = self.mine(j, 1 - e, p.mod(p.i1 + DIRS[e]), b).astype(bf)
        elif k == 2:
            for e in BOTH:
                for b in range(n):
                    o[out, e, b] = (self.got(0)[j, e, 0, b].astype(f32) + self.mine(j, e, p.mod(p.i1 + DIRS[e]), b)).astype(bf)
        elif k == 3:
            for h in BOTH:
                for b in range(n):
                    self.mid[m, h, b] = self.got(1)[j, h, b].astype(f32) + self.got(0)[j, 1 - h, 1, b].astype(f32) + self.mine(j, h, p.i1, b)
            for e in BOTH:
                o[out, e, 0] = self.mid[m, e, p.mod(p.i2 + 2)].astype(bf)
                o[out, e, 1] = self.mid[m, 1 - e, p.mod(p.i2 + DIRS[e])].astype(bf)
        elif k == 4:
            for e in BOTH:
                o[out, e] = (self.got(2)[j, e, 0].astype(f32) + self.mid[m, e, p.mod(p.i2 + DIRS[e])]).astype(bf)
        else:
            for h in BOTH:
                self.done(j, h, self.got(3)[j, h].astype(f32) + self.got(2)[j, 1 - h, 1].astype(f32) + self.mid[m, h, p.i2])
        if k < 5:
            for e in BOTH:
                self.copy(k - 1, j, e).start()


def scatter_slots(m, lag):
    return min(m, 3 * lag), min(m, lag)


def scatter_bufs(m, lag, side, R, C):
    keep, pool = scatter_slots(m, lag)
    few, V, D = min(m, lag), pltpu.VMEM, pltpu.SemaphoreType.DMA
    pairs = [V((k, 2, *s, R, C), bf) for s in ((2, side), (side,), (2,), ()) for k in (few, m)]
    return [V((keep + pool, 2, side * side, R, C), bf), V((m, 2, side * side, R, C), bf), V((min(m, 2 * lag), 2, side, R, C), f32), *pairs,
            D((m,)), D((m,)), D((m, 4, 2)), D((m, 4, 2))]


def normed_rows(h):
    wide = h.astype(f32)
    scale = lax.rsqrt(jnp.mean(wide * wide, -1, keepdims=True) + 1e-6)
    return (wide * scale).astype(bf)


def forward(n, x, dy, wg, wu, wd, lag=2, cg=256, cd=128, cid=1):
    side = math.isqrt(n // 2)
    T, Dm = x.shape
    L, R, F = wg.shape
    Rd = wd.shape[1]
    ng, nd, rows, tile = F // cg, Dm // (2 * cd), T // 2, T // 8
    width = 2 * cd

    def kernel(x_h, dy_h, wg_ref, wu_ref, wd_ref, ogu, od, g0, u0, act0, h1, a0, a1, act1, dgu1,
               xv, av, dyv, actv, own_v, wb, wdb, wdr, stg, st3, s_in, s_w, s_wd, s_wr, s_stg, s_act, s_out, s_st3, *sems):
        p = Place(n)
        pltpu.make_async_copy(x_h, xv, s_in.at[0]).start()
        pltpu.make_async_copy(dy_h, dyv, s_in.at[1]).start()
        own_v[:, 0] = wg_ref[...]
        own_v[:, 1] = wu_ref[...]
        barrier(p)
        every = slice(None)

        def cols(j, w):
            return pl.ds(pl.multiple_of(j * w, w), w)
        def core_rows(c):
            return pl.ds(c * Rd if isinstance(c, int) else pl.multiple_of(c * Rd, 8), Rd)
        def place(q, m):
            return q // m, lax.rem(q, m)

        def at_g(q, e, x, y, c):
            l, j = place(q, ng)
            return ogu.at[l, x, y, c, every if e is None else e, every, cols(j, cg)]
        def at_d(q, e, x, y, c):
            l, j = place(q, nd)
            return od.at[l, x, y, core_rows(c), cols(j, width) if e is None else cols(2 * j + e, cd)]
        def own_g(q):
            l, j = place(q, ng)
            return own_v.at[l, every, every, cols(j, cg)]
        def own_d(q):
            l, j = place(q, nd)
            return wd_ref.at[l, every, cols(j, width)]

        def stream(at, own, sent, local, sems):
            x, y = p.i1 + p.c * (p.i2 - p.i1), p.i2 + p.c * (p.i1 - p.i2)
            def block(q, e, j1, j2):
                return at(q, e, j1 + p.c * (j2 - j1), j2 + p.c * (j1 - j2), p.c)
            def row(q, e, core, j2):
                return at(q, e, j2, every, core) if core else at(q, e, every, j2, core)
            def core(q, c):
                return at(q, None, every, every, c)
            return Gather(p, own, block, row, core, sent, local(x, y), sems)

        r0, h0 = core_rows(0), pl.ds(0, Dm // 2)
        sent_g = [ogu.at[:, 0, 0, 0], ogu.at[:, 0, 0, 0, 0], ogu.at[:, :, 0, 0], ogu.at[:, :, 0, 0, 0], ogu.at[:, :, :, 0]]
        sent_d = [od.at[:, 0, 0, r0], od.at[:, 0, 0, r0, h0], od.at[:, :, 0, r0], od.at[:, :, 0, r0, h0], od.at[:, :, :, r0]]
        G = stream(at_g, own_g, sent_g, lambda x, y: [(own_v.at[l], ogu.at[l, x, y, p.c]) for l in range(L)], sems[:5])
        Ds = stream(at_d, own_d, sent_d, lambda x, y: [(wd_ref.at[l], od.at[l, x, y, core_rows(p.c)]) for l in range(L)], sems[5:])
        G.begin()
        Ds.begin()
        downs = 2 * nd
        chunks, depth = 2 * ng + downs, (Gather.STAGES - 1) * lag

        def load_g(q):
            l, j = place(q, ng)
            return pltpu.make_async_copy(ogu.at[l, :, :, :, :, :, cols(j, cg)], wb.at[lax.rem(q, 2)], s_w.at[lax.rem(q, 2)])
        def load_d(j):
            return pltpu.make_async_copy(od.at[0, :, :, :, cols(j, width)], wdb.at[lax.rem(j, 2)], s_wd.at[lax.rem(j, 2)])
        def load_r(k):
            return pltpu.make_async_copy(od.at[1, k // side, lax.rem(k, side)], wdr.at[pl.ds(pl.multiple_of(k * 2 * Rd, 2 * Rd), 2 * Rd)], s_wr.at[k])
        def weights(q, e):
            return wb[lax.rem(q, 2), :, :, :, e].reshape(Dm, cg)
        def part(r):
            return pl.ds(pl.multiple_of(r * rows, rows), rows)
        def put_g(j, r):
            return [pltpu.make_async_copy(stg.at[r, e], (g0, u0)[e].at[part(r), cols(j, cg)], s_stg.at[r, e]) for e in BOTH]
        def put_act(j):
            return pltpu.make_async_copy(actv.at[:, cols(j, cg)], act0.at[:, cols(j, cg)], s_act.at[j])
        def put_3(j, r):
            to = [act1.at[part(r), cols(j, cg)], *(dgu1.at[e, part(r), cols(j, cg)] for e in BOTH)]
            return [pltpu.make_async_copy(st3.at[r, e], ref, s_st3.at[r, e]) for e, ref in enumerate(to)]
        put_a0 = pltpu.make_async_copy(av, a0, s_out.at[0])
        put_h1 = pltpu.make_async_copy(xv, h1, s_out.at[1])
        put_a1 = pltpu.make_async_copy(av, a1, s_out.at[2])

        def norm():
            def one(r, _):
                rs_ = pl.ds(pl.multiple_of(r * tile, tile), tile)
                av[rs_, :] = normed_rows(xv[rs_, :])
                return 0
            lax.fori_loop(0, T // tile, one, 0)

        def first():
            pltpu.make_async_copy(x_h, xv, s_in.at[0]).wait()
            pltpu.make_async_copy(dy_h, dyv, s_in.at[1]).wait()
            norm()
            put_a0.start()

        def gate_up(j):
            load_g(j).wait()
            def one(r, _):
                @pl.when(j > 0)
                def _():
                    for c in put_g(j - 1, r):
                        c.wait()
                a = av[part(r), :]
                g = jnp.dot(a, weights(j, 0), preferred_element_type=f32)
                u = jnp.dot(a, weights(j, 1), preferred_element_type=f32)
                s = jax.nn.sigmoid(g)
                gs = g * s
                stg[r, 0] = u * (s + gs * (1.0 - s))
                stg[r, 1] = gs
                actv[part(r), cols(j, cg)] = (gs * u).astype(bf)
                for c in put_g(j, r):
                    c.start()
                return 0
            lax.fori_loop(0, 2, one, 0)
            put_act(j).start()

        def down(j):
            load_d(j).wait()
            def one(r, _):
                y = jnp.dot(actv[part(r), :], wdb[lax.rem(j, 2)].reshape(F, width), preferred_element_type=f32).astype(bf)
                xv[part(r), cols(j, width)] = xv[part(r), cols(j, width)] + y
                return 0
            lax.fori_loop(0, 2, one, 0)

        def second():
            for r in BOTH:
                for c in put_g(ng - 1, r):
                    c.wait()
            put_a0.wait()
            put_h1.start()
            norm()
            put_a1.start()

        def gate_up_back(j):
            load_g(ng + j).wait()
            @pl.when(j == 0)
            def _():
                def wait(k, _):
                    load_r(k).wait()
                    return 0
                lax.fori_loop(0, side * side, wait, 0)
            def one(r, _):
                @pl.when(j > 0)
                def _():
                    for c in put_3(j - 1, r):
                        c.wait()
                a = av[part(r), :]
                g = jnp.dot(a, weights(ng + j, 0), preferred_element_type=f32)
                u = jnp.dot(a, weights(ng + j, 1), preferred_element_type=f32)
                d = lax.dot_general(dyv[part(r), :], wdr[cols(j, cg), :], NT, preferred_element_type=f32).astype(bf).astype(f32)
                s = jax.nn.sigmoid(g)
                gs = g * s
                st3[r, 0] = (gs * u).astype(bf)
                st3[r, 1] = (d * u * (s + gs * (1.0 - s))).astype(bf)
                st3[r, 2] = (d * gs).astype(bf)
                for c in put_3(j, r):
                    c.start()
                return 0
            lax.fori_loop(0, 2, one, 0)

        def tick(t, _):
            for k in reversed(range(Gather.STAGES)):
                q = t - k * lag
                late = q >= ng + downs
                @pl.when((q >= 0) & (q < chunks) & ((q < ng) | late))
                def _():
                    j = q - jnp.where(late, downs, 0)
                    G.stage(k, j)
                    if k == Gather.STAGES - 1:
                        load_g(j).start()
                @pl.when((q >= ng) & (q < ng + downs))
                def _():
                    j = q - ng
                    Ds.stage(k, j)
                    if k == Gather.STAGES - 1:
                        @pl.when(j < nd)
                        def _():
                            load_d(j).start()
                        @pl.when(j == downs - 1)
                        def _():
                            def start(k, _):
                                load_r(k).start()
                                return 0
                            lax.fori_loop(0, side * side, start, 0)
            @pl.when(t == min(2, lag - 1))
            def _():
                first()
            m = t - depth - 1
            @pl.when((m >= 0) & (m < ng))
            def _():
                gate_up(m)
            @pl.when((m >= ng) & (m < ng + nd))
            def _():
                down(m - ng)
            @pl.when(m == ng + nd)
            def _():
                second()
            @pl.when(m >= ng + downs)
            def _():
                gate_up_back(m - ng - downs)
            return 0
        lax.fori_loop(0, chunks + depth + 1, tick, 0)
        for r in BOTH:
            for c in put_3(ng - 1, r):
                c.wait()
        G.end()
        Ds.end()
        def last(j, _):
            put_act(j).wait()
            return 0
        lax.fori_loop(0, ng, last, 0)
        put_h1.wait()
        put_a1.wait()

    S, V, A, D = jax.ShapeDtypeStruct, pl.BlockSpec(memory_space=pltpu.VMEM), pl.BlockSpec(memory_space=pl.ANY), pltpu.SemaphoreType.DMA
    VM = pltpu.VMEM
    sems = gather_sems(L * ng, L) + gather_sems(L * nd, L)
    wide, thin = S((T, F), bf), S((T, Dm), bf)
    out = pl.pallas_call(
        kernel, name="forward",
        out_shape=[S((L, side, side, 2, 2, R, F), bf), S((L, side, side, 2 * Rd, Dm), bf),
                   S((T, F), f32), S((T, F), f32), wide, thin, thin, thin, wide, S((2, T, F), bf)],
        in_specs=[A, A, V, V, V], out_specs=[A] * 10,
        scratch_shapes=[VM((T, Dm), bf), VM((T, Dm), bf), VM((T, Dm), bf), VM((T, F), bf), VM((L, 2, R, F), bf), VM((2, side, side, 2, 2, R, cg), bf), VM((2, side, side, 2 * Rd, width), bf), VM((F, Dm), bf),
                        VM((2, 2, rows, cg), f32), VM((2, 3, rows, cg), bf),
                        D((2,)), D((2,)), D((2,)), D((side * side,)), D((2, 2)), D((ng,)), D((3,)), D((2, 3)), *sems],
        compiler_params=pltpu.CompilerParams(collective_id=cid, has_side_effects=True, vmem_limit_bytes=67043328),
    )(x, dy, wg, wu, wd)
    ogu, od, *rest = out
    return ogu, od.reshape(L, n * Rd, Dm), *rest


def greet_all(n):
    me, sem = lax.axis_index("dp"), pltpu.get_barrier_semaphore()
    def greet(k, _):
        pl.semaphore_signal(sem, inc=1, device_id={"dp": lax.rem(me + k, n)}, device_id_type=MESH)
        return 0
    lax.fori_loop(1, n, greet, 0)
    pl.semaphore_wait(sem, n - 1)


def clip(n, count, part, o_ref, x_ref, got, send, recv):
    me = lax.axis_index("dp")
    x_ref[...] = part
    def copy(k, slot):
        return pltpu.make_async_remote_copy(src_ref=x_ref, dst_ref=got.at[slot], send_sem=send.at[k], recv_sem=recv.at[slot], device_id={"dp": lax.rem(me + k, n)}, device_id_type=MESH)
    def start(k, _):
        copy(k, me).start()
        return 0
    lax.fori_loop(1, n, start, 0)
    got[me] = part
    def wait(k, _):
        copy(k, me).wait_send()
        copy(k, lax.rem(me + k, n)).wait_recv()
        return 0
    lax.fori_loop(1, n, wait, 0)
    o_ref[...] = jnp.minimum(1.0, 0.5 * lax.rsqrt(jnp.full_like(part, jnp.sum(got[...])) / count + 1e-30))


def update(factor, weights, moments, squares, grads):
    L = len(grads)
    def kernel(f_ref, *refs):
        f, layer = f_ref[0, 0], pl.program_id(0)
        ins, outs = refs[:-9], refs[-9:]
        for i in range(3):
            w, m, v = (ins[3 * k + i][0].astype(jnp.float32) for k in range(3))
            g = ins[9 + i][...].astype(jnp.float32)
            for l in range(1, L):
                g = jnp.where(layer == l, ins[9 + 3 * l + i][...].astype(jnp.float32), g)
            g = g * f
            m = 0.9 * m + 0.1 * g
            v = 0.95 * v + 0.05 * g * g
            step = m * lax.rsqrt(v + 1e-8) + 0.1 * w
            outs[i][0] = (w - 0.02 * step).astype(bf)
            outs[3 + i][0] = m
            outs[6 + i][0] = v
    def whole(a):
        return pl.BlockSpec((1, a.shape[1], a.shape[2] // 2), lambda l, c: (l, 0, c))
    arrays = (*weights, *moments, *squares)
    flat = [g for layer in grads for g in layer]
    S = jax.ShapeDtypeStruct
    return pl.pallas_call(
        kernel, name="update", grid=(L, 2),
        out_shape=[S(a.shape, a.dtype) for a in arrays],
        in_specs=[pl.BlockSpec(memory_space=pltpu.SMEM), *map(whole, arrays), *(pl.BlockSpec((g.shape[0], g.shape[1] // 2), lambda l, c: (0, c)) for g in flat)],
        out_specs=[*map(whole, arrays)],
    )(factor, *arrays, *flat)


class Layer:
    def __init__(self, n, a, act, lag, lagd, cg, cd):
        self.n, self.side = n, math.isqrt(n // 2)
        self.T, self.Dm = a.shape
        self.F = act.shape[1]
        self.R, self.Rd, self.ng, self.nd = self.Dm // n, self.F // n, self.F // cg, self.Dm // (2 * cd)
        self.lag, self.lagd, self.cg, self.cd, self.half, self.chips = lag, lagd, cg, cd, self.F // 2, self.side * self.side
    def bufs(self):
        return [*scatter_bufs(self.nd, self.lagd, self.side, self.Rd, self.cd), *scatter_bufs(self.ng, self.lag, self.side, self.R, self.cg)]
    def outs(self):
        S = jax.ShapeDtypeStruct
        return [S((self.R, self.F), bf), S((self.R, self.F), bf), S((self.Rd, self.Dm), bf), S((8, 128), f32)]
    def streams(self, p, og, ou, od, sq, bufs):
        def add(v):
            w = v.astype(f32)
            w = jnp.sum((w * w).reshape(w.shape[0] // 8, 8, w.shape[1]), 0)
            for k in range(w.shape[1] // 128):
                sq[...] += w[:, 128 * k:128 * k + 128]
        def done_d(j, e, v):
            v = v.astype(bf)
            od[:, pl.ds(pl.multiple_of((2 * j + e) * self.cd, self.cd), self.cd)] = v
            add(v)
        def done_g(j, e, v):
            v = v.astype(bf)
            (og, ou)[e][:, pl.ds(pl.multiple_of(j * self.cg, self.cg), self.cg)] = v
            add(v)
        sq[...] = jnp.zeros_like(sq)
        self.p = p
        split = len(bufs) // 2
        self.sd = Scatter(p, self.lagd, bufs[:split], done_d)
        self.sg = Scatter(p, self.lag, bufs[split:], done_g)
    def put_d(self, j, m, val):
        for e in BOTH:
            v = val[:, e * self.cd:(e + 1) * self.cd].reshape(self.chips // 2, 2, self.Rd, self.cd).astype(bf)
            for h in BOTH:
                self.sd.own[self.sd.slot(j, h), e, m * self.chips // 2:(m + 1) * self.chips // 2] = v[:, h]
    def put_g(self, j, val):
        for e in BOTH:
            v = val[:, e * self.cg:(e + 1) * self.cg].reshape(self.chips, 2, self.R, self.cg).astype(bf)
            for h in BOTH:
                self.sg.own[self.sg.slot(j, h), e] = v[:, h]
    def run(self, make_d, make_g, extra=0, more=None):
        streams = ((self.sd, self.nd, 0, self.lagd, make_d), (self.sg, self.ng, self.nd, self.lag, make_g))
        total = max(lo + m + (Scatter.STAGES - 1) * lg for _, m, lo, lg, _ in streams)
        total = max(total, self.nd + self.ng + extra)
        def body(i, _):
            for k in reversed(range(Scatter.STAGES)):
                for s, m, lo, lg, make in streams:
                    j = i - lo - k * lg
                    @pl.when((j >= 0) & (j < m))
                    def _():
                        make(j) if k == 0 else s.stage(k, j)
            if extra:
                j = i - self.nd - self.ng
                @pl.when((j >= 0) & (j < extra))
                def _():
                    more(j)
            return 0
        lax.fori_loop(0, total, body, 0)


def pieces(half, most=768):
    return [(m, lo, min(lo + most, (m + 1) * half)) for m in BOTH for lo in range(m * half, (m + 1) * half, most)]


def load_pieces(src, dst, half, sem):
    return [(m, pltpu.make_async_copy(src.at[:, lo:hi], dst.at[:src.shape[0], lo:hi], sem.at[k])) for k, (m, lo, hi) in enumerate(pieces(half))]


def down_products(k, j, act, rhs, loads):
    for m in BOTH:
        @pl.when(j == 0)
        def _():
            for which, c in loads:
                if which == m:
                    c.wait()
        k.put_d(j, m, jnp.concatenate([lax.dot_general(act[:k.T, lo:hi], rhs, TN, preferred_element_type=f32) for which, lo, hi in pieces(k.half) if which == m], 0))


def cols_of(j, w):
    return pl.ds(pl.multiple_of(j * w, w), w)


def backward_last(n, a, act, dgu, dy, h, wgu, layer, lag=2, lagd=2, cg=256, cd=128, cid=2):
    k = Layer(n, a, act, lag, lagd, cg, cd)
    T, Dm, F, tile = k.T, k.Dm, k.F, k.T // k.nd
    def kernel(a_h, act_h, dgu_h, dy_h, h_h, w_h, og, ou, od, sq, dh_h,
               a_v, act_v, dg_v, dy_v, row_v, part_v, ld, ldg, ldy, ldr, ldo, ldw, *bufs):
        p = Place(n)
        act_loads = load_pieces(act_h, act_v, k.half, ld)
        load_a = pltpu.make_async_copy(a_h, a_v, ldw)
        def load_dy(j):
            return pltpu.make_async_copy(dy_h.at[:, cols_of(j, 2 * cd)], dy_v.at[lax.rem(j, 2)], ldy.at[lax.rem(j, 2)])
        def load_dg(j, e):
            return pltpu.make_async_copy(dgu_h.at[e, :, cols_of(j, cg)], dg_v.at[lax.rem(j, 2), :, e * cg:(e + 1) * cg], ldg.at[lax.rem(j, 2), e])
        def load_w(d):
            for e in BOTH:
                chip = d // 2
                rows = pl.ds(pl.multiple_of((e * n + d) * k.R, k.R), k.R)
                pltpu.make_async_copy(w_h.at[layer, chip // k.side, lax.rem(chip, k.side), lax.rem(d, 2), e], act_v.at[rows], ldw).start()
            return 0
        w_v = act_v.at[:2 * Dm]
        def load_row(r, e):
            return pltpu.make_async_copy(dgu_h.at[e, cols_of(r, tile), :], row_v.at[e], ldr.at[e])
        def blocks(ref, r, v):
            return [(ref.at[cols_of(r, tile), c * 2 * cd:(c + 1) * 2 * cd], v.at[c * tile:(c + 1) * tile]) for c in range(k.nd)]
        h_v, y_v = dy_v.at[0], dy_v.at[1]
        def load_tile(ref, r, v, sem):
            for src, dst in blocks(ref, r, v):
                pltpu.make_async_copy(src, dst, sem).start()
        def load_h(r):
            load_tile(h_h, r, h_v, ldr.at[2])
        def load_y(r):
            load_tile(dy_h, r, y_v, ldr.at[3])
        def put(r):
            for dst, src in blocks(dh_h, r, y_v):
                pltpu.make_async_copy(src, dst, ldo).start()
        def arrived(v, sem):
            pltpu.make_async_copy(v, v, sem).wait()
        def tile_of(v, m):
            return jnp.concatenate([v[pl.ds(pl.multiple_of(c * tile + m * part, part), part)] for c in range(k.nd)], 1)
        part = tile // 4
        load_dy(0).start()
        for _, c in act_loads:
            c.start()
        barrier(p)
        k.streams(p, og, ou, od, sq, bufs)
        load_dy(0).wait()
        def make_d(j):
            @pl.when(j + 1 < k.nd)
            def _(): load_dy(j + 1).start()
            @pl.when(j == 0)
            def _(): load_a.start()
            @pl.when(j == k.nd - 1)
            def _():
                for e in BOTH: load_dg(0, e).start()
            down_products(k, j, act_v, dy_v[lax.rem(j, 2)], act_loads)
            k.sd.send(j)
            @pl.when(j + 1 < k.nd)
            def _(): load_dy(j + 1).wait()
        def make_g(j):
            @pl.when(j + 1 < k.ng)
            def _():
                for e in BOTH: load_dg(j + 1, e).start()
            @pl.when(j == 0)
            def _():
                load_a.wait()
                lax.fori_loop(0, n, lambda d, _: load_w(d), 0)
            @pl.when(j == k.ng - 1)
            def _():
                for e in BOTH: load_row(0, e).start()
                load_h(0)
                load_y(0)
            for e in BOTH:
                load_dg(j, e).wait()
            k.put_g(j, lax.dot_general(a_v[...], dg_v[lax.rem(j, 2)], TN, preferred_element_type=f32))
            k.sg.send(j)
        def rows(i):
            r, e, s = i // 4, lax.rem(i // 2, 2), lax.rem(i, 2)
            wide = Dm // 2
            @pl.when(i == 0)
            def _():
                pltpu.make_async_copy(w_v, w_v, ldw).wait()
            @pl.when((e == 0) & (s == 0) & (r > 0))
            def _():
                arrived(y_v, ldo)
                load_y(r)
            @pl.when(s == 0)
            def _():
                load_row(r, e).wait()
            some = pl.ds(pl.multiple_of(s * wide, wide), wide)
            part_v[e, :, some] = lax.dot_general(row_v[e], act_v[pl.ds(pl.multiple_of(e * Dm + s * wide, wide), wide)], NT, preferred_element_type=f32).astype(bf)
            @pl.when((s == 1) & (r + 1 < T // tile))
            def _():
                load_row(r + 1, e).start()
            @pl.when((e == 1) & (s == 1))
            def _():
                arrived(h_v, ldr.at[2])
                arrived(y_v, ldr.at[3])
                def one(m, _):
                    some = cols_of(m, part)
                    da = (part_v[0, some] + part_v[1, some]).astype(f32)
                    wide = tile_of(h_v, m).astype(f32)
                    s = lax.rsqrt(jnp.mean(wide * wide, -1, keepdims=True) + 1e-6)
                    t = jnp.sum(da * wide, -1, keepdims=True) * (s * s * s) * (1.0 / Dm)
                    new = (da * s - wide * t).astype(bf) + tile_of(y_v, m)
                    for c in range(k.nd):
                        y_v[pl.ds(pl.multiple_of(c * tile + m * part, part), part)] = new[:, c * 2 * cd:(c + 1) * 2 * cd]
                    return 0
                lax.fori_loop(0, 4, one, 0)
                put(r)
                @pl.when(r + 1 < T // tile)
                def _():
                    load_h(r + 1)
        k.run(make_d, make_g, 4 * (T // tile), rows)
        arrived(y_v, ldo)
    V, A, D, VM = pl.BlockSpec(memory_space=pltpu.VMEM), pl.BlockSpec(memory_space=pl.ANY), pltpu.SemaphoreType.DMA, pltpu.VMEM
    return pl.pallas_call(
        kernel, name="backward_last", out_shape=[*k.outs(), jax.ShapeDtypeStruct((T, Dm), bf)], in_specs=[A] * 6, out_specs=[V] * 4 + [A],
        scratch_shapes=[VM((T, Dm), bf), VM((max(T, 2 * Dm), F), bf), VM((2, T, 2 * cg), bf), VM((2, T, 2 * cd), bf), VM((2, tile, F), bf), VM((2, tile, Dm), bf),
                        D((4,)), D((2, 2)), D((2,)), D((4,)), D, D, *k.bufs()],
        compiler_params=pltpu.CompilerParams(collective_id=cid, has_side_effects=True, vmem_limit_bytes=67043328),
    )(a, act, dgu, dy, h, wgu)


def backward_first(n, a, act, by_gate, by_up, dh, wd, sq_last, count, layer, lag=2, lagd=2, cg=256, cd=128, cid=3):
    k = Layer(n, a, act, lag, lagd, cg, cd)
    T, Dm, F, rows = k.T, k.Dm, k.F, k.T // 2
    def kernel(a_h, act_h, g_h, u_h, dh_h, wd_h, sq_ref, og, ou, od, factor, a_v, act_v, gu_v, dg_v, dh_v, wd_v, ld, ldg, ldw, ldh, sq, part_v, got, send, recv, *bufs):
        p = Place(n)
        act_loads = load_pieces(act_h, act_v, k.half, ld)
        load_a = pltpu.make_async_copy(a_h, a_v, ldw)
        def load_dh(j):
            cols = cols_of(j, 2 * cd)
            return pltpu.make_async_copy(dh_h.at[:, cols], dh_v.at[:, cols], ldh.at[j])
        def part(r):
            return pl.ds(pl.multiple_of(r * rows, rows), rows)
        def load_gu(j, r):
            return [pltpu.make_async_copy((g_h, u_h)[e].at[part(r), cols_of(j, cg)], gu_v.at[r, e], ldg.at[r, e]) for e in BOTH]
        def load_wd(j):
            return pltpu.make_async_copy(wd_h.at[layer, cols_of(j, cg), :], wd_v, ldw)
        load_dh(0).start()
        for _, c in act_loads:
            c.start()
        for j in range(1, k.nd):
            load_dh(j).start()
        greet_all(n)
        k.streams(p, og, ou, od, sq, bufs)
        def make_d(j):
            @pl.when(j == 0)
            def _(): load_a.start()
            @pl.when(j == k.nd - 1)
            def _():
                for r in BOTH:
                    for c in load_gu(0, r): c.start()
                load_a.wait()
                load_wd(0).start()
            load_dh(j).wait()
            down_products(k, j, act_v, dh_v[:, cols_of(j, 2 * cd)], act_loads)
            k.sd.send(j)
        def make_g(j):
            load_wd(j).wait()
            def one(r, _):
                for c in load_gu(j, r):
                    c.wait()
                d = lax.dot_general(dh_v[part(r), :], wd_v[...], NT, preferred_element_type=f32).astype(bf).astype(f32)
                for e in BOTH:
                    dg_v[part(r), e * cg:(e + 1) * cg] = (d * gu_v[r, e]).astype(bf)
                @pl.when(j + 1 < k.ng)
                def _():
                    for c in load_gu(j + 1, r): c.start()
                return 0
            lax.fori_loop(0, 2, one, 0)
            @pl.when(j + 1 < k.ng)
            def _():
                load_wd(j + 1).start()
            k.put_g(j, lax.dot_general(a_v[...], dg_v[...], TN, preferred_element_type=f32))
            k.sg.send(j)
        k.run(make_d, make_g)
        clip(n, count, sq[...] + sq_ref[...], factor, part_v, got, send, recv)
    V, A, D, VM = pl.BlockSpec(memory_space=pltpu.VMEM), pl.BlockSpec(memory_space=pl.ANY), pltpu.SemaphoreType.DMA, pltpu.VMEM
    return pl.pallas_call(
        kernel, name="backward_first", out_shape=k.outs(), in_specs=[A] * 6 + [V], out_specs=[V] * 4,
        scratch_shapes=[VM((T, Dm), bf), VM((T, F), bf), VM((2, 2, rows, cg), f32), VM((T, 2 * cg), bf), VM((T, Dm), bf), VM((cg, Dm), bf),
                        D((4,)), D((2, 2)), D, D((k.nd,)), VM((8, 128), f32), VM((8, 128), f32), VM((n, 8, 128), f32), D((n,)), D((n,)), *k.bufs()],
        compiler_params=pltpu.CompilerParams(collective_id=cid, has_side_effects=True, vmem_limit_bytes=67043328),
    )(a, act, by_gate, by_up, dh, wd, sq_last)


def solution(mesh):
    n = mesh.shape["dp"]

    def step(x, dy, *arrays):
        weights, m, v = (arrays[i : i + 3] for i in (0, 3, 6))
        x, dy = x[0], dy[0]
        wgu, wd, g0, u0, act0, h1, a0, a1, act1, dgu1 = forward(n, x, dy, *weights)
        *mine1, sq1, dh1 = backward_last(n, a1, act1, dgu1, dy, h1, wgu, 1)
        *mine0, factor = backward_first(n, a0, act0, g0, u0, dh1, wd, sq1, n * sum(w.size for w in weights), 0)
        return tuple(update(factor, weights, m, v, (mine0, mine1)))

    states, cut = P(("rep", "dp"), None, None), P(None, "dp", None)
    return jax.shard_map(
        step,
        mesh=mesh,
        in_specs=(states, states) + (cut,) * 9,
        out_specs=(P("rep", "dp", None),) * 9,
        check_vma=False,
    )
```
